32 devices in a mesh: dp: 2 (over x), mode: 4 (over z), tm: 4 (over y, core).
Axes of the slice: x: 2, y: 2, z: 4, core: 2. Of those that a mesh axis runs over, the one named last changes fastest.
Arguments:
- input_field: float32 [2, 16, 8, 16384], P(None, 'dp', 'mode', 'tm'), parts along dimension 1, may hold values from -6 to 6
- target_field: float32 [2, 16, 8, 16384], P(None, 'dp', 'mode', 'tm'), parts along dimension 1, may hold values from -6 to 6
- margin: float32 [8, 8, 16], P('mode'), may hold values from -0.5 to 0.5
- pair_index: int32 [16, 2], replicated, may hold values from 0 to 7
- mode_beta: float32 [1024, 8, 3], P(None, 'mode'), may hold values from -2 to 2
- segment_kind: int32 [1], replicated, may hold values from 0 to 1023
Outputs:
- field_gradient: float32 [2, 16, 8, 16384], P(None, 'dp', 'mode', 'tm'), parts along dimension 1
The draws below stay inside these ranges and needn't reach their ends.
There are 2 independent parts, one for each index of `dp`. The reference program is written for one: setup_inputs(seed, part) draws one part's arguments, and reference() takes and returns one part's arrays. A program takes and returns all parts, laid end to end along the dimension named above; an argument that names none is the same for every part. Nothing has to cross between parts.
All inputs are finite; a program needn't handle non-finite values.
Results may differ from the reference program's by a relative error of at most 0.00011.
Values sent between devices are 32-bit elements; how exact they have to be, the bound alone decides.
A program may use at most 128 MiB of HBM per device.

```python
import jax
import jax.numpy as jnp
from jax import lax

PULSES = 8
NT = 16384
PAIRS = 16
STEPS = 1
KINDS = 1024
MODES = 8


def set_ends(array, own_key, low, largest):
    spot = [jax.random.randint(jax.random.fold_in(own_key, axis), (), 0, length) for axis, length in enumerate(array.shape)]
    widest = array.shape.index(max(array.shape))
    neighbour = spot[:widest] + [(spot[widest] + 1) % array.shape[widest]] + spot[widest + 1:]
    return array.at[tuple(spot)].set(low).at[tuple(neighbour)].set(largest)


def steps_of(rng, dims, split, low, high):
    factor_of, own = 1.0, jax.random.fold_in(rng, 6)
    for dim, blocks in split:
        heights = jnp.exp(jax.random.uniform(jax.random.fold_in(own, dim), (blocks,), jnp.float32, low / len(split), high / len(split)))
        factor_of = factor_of * jnp.repeat(heights, dims[dim] // blocks).reshape([-1 if axis == dim else 1 for axis in range(len(dims))])
    return factor_of


def normal_values(stream_key, shape, spread, most, shards=(), kind=jnp.bfloat16):
    drawn = jax.random.normal(stream_key, shape, jnp.float32) * spread
    if len(shards) > 0:
        drawn = steps_of(stream_key, shape, shards, -0.22, 0.18) * drawn
    return jnp.clip(drawn, min=-most, max=most).astype(kind)


def setup_inputs(seed: int = 0, part: int = 0) -> dict:
    key_list = jax.random.split(jax.random.key(seed), 7)
    own_keys = jax.random.split(jax.random.fold_in(key_list[6], part), 7)
    input_field = normal_values(own_keys[0], (2, PULSES, MODES, NT), 1.0, 6.0, ((2, 4), (3, 4)), jnp.float32)
    target_field = normal_values(own_keys[1], (2, PULSES, MODES, NT), 1.0, 6.0, ((2, 4), (3, 4)), jnp.float32)
    margin = normal_values(key_list[2], (MODES, MODES, PAIRS), (MODES * PAIRS) ** -0.5, 0.5, ((0, 4),), jnp.float32)
    pair_index = set_ends(jax.random.randint(key_list[3], (PAIRS, 2), 0, MODES), jax.random.fold_in(key_list[3], 1), 0, MODES - 1).astype(jnp.int32)
    mode_beta = jnp.clip(jax.random.uniform(key_list[4], (KINDS, MODES, 3), jnp.float32, -2.0, 2.0) * steps_of(key_list[4], (KINDS, MODES, 3), ((1, 4),), -0.4, 0.0), -2.0, 2.0)
    segment_kind = jax.random.randint(key_list[5], (STEPS,), 0, KINDS).astype(jnp.int32)
    return dict(input_field=input_field, target_field=target_field, margin=margin, pair_index=pair_index, mode_beta=mode_beta, segment_kind=segment_kind)


kerr_scale = 0.1

def phases(mode_table):
    index = jnp.arange(NT, dtype=jnp.int32)
    signed = jnp.where(index < NT // 2, index, index - NT).astype(jnp.float32)
    omega = signed * (8.0 / NT)
    return mode_table[:, 0:1] * omega + mode_table[:, 1:2] * omega ** 2 / 2.0 + mode_table[:, 2:3] * omega ** 3 / 6.0

def disperse(pulse_field, phase):
    values = pulse_field[0] + 1j * pulse_field[1]
    spectrum = jnp.fft.fft(values, axis=-1) * jnp.exp(1j * phase)[None]
    result = jnp.fft.ifft(spectrum, axis=-1)
    return jnp.stack([jnp.real(result), jnp.imag(result)])

def nonlinear(pulse_field, margin, pair_index):

    def single(pulse):
        left = pulse[:, pair_index[:, 0], :]
        right = pulse[:, pair_index[:, 1], :]
        prod_real = left[0] * right[0] - left[1] * right[1]
        prod_imag = left[0] * right[1] + left[1] * right[0]
        coup_real = jnp.einsum('pnj,js->pns', margin, prod_real, precision=lax.Precision.HIGHEST)
        coup_imag = jnp.einsum('pnj,js->pns', margin, prod_imag, precision=lax.Precision.HIGHEST)
        non_real = lax.optimization_barrier(jnp.sum(coup_real * pulse[0][None] + coup_imag * pulse[1][None], axis=1))
        non_imag = lax.optimization_barrier(jnp.sum(coup_imag * pulse[0][None] - coup_real * pulse[1][None], axis=1))
        return jnp.stack([-kerr_scale * non_imag, kerr_scale * non_real])
    mapped = lax.map(single, jnp.moveaxis(pulse_field, 1, 0))
    return jnp.moveaxis(mapped, 0, 1)

def forward(pulse_field, margin, pair_index, mode_beta, segment_kind):
    for segment in range(STEPS):
        phase = phases(mode_beta[segment_kind[segment]])
        pulse_field = disperse(pulse_field, phase)
        pulse_field = pulse_field + nonlinear(pulse_field, margin, pair_index)
    return pulse_field

def reference(input_field, target_field, margin, pair_index, mode_beta, segment_kind):

    def misfit(pulse_field):
        output_field = forward(pulse_field, margin, pair_index, mode_beta, segment_kind)
        return jnp.sum((output_field - target_field) ** 2)
    value, pullback = jax.vjp(misfit, input_field)
    gradient = pullback(jnp.ones_like(value))[0]
    return gradient
```

```python
import functools
import math

import jax
import jax.numpy as jnp
import numpy as np
from jax import lax
from jax.experimental import pallas as pl
from jax.experimental.pallas import tpu as pltpu
from jax.sharding import PartitionSpec as P

kerr_scale = 0.1
MESH = pl.DeviceIdType.MESH
f32 = jnp.float32
bf16 = jnp.bfloat16


def split_table(table):
    high = table.astype(np.float32).astype(bf16)
    low = (table - high.astype(np.float64)).astype(np.float32).astype(bf16)
    return np.stack([np.asarray(high), np.asarray(low)])


def real_form(size):
    turns = np.outer(np.arange(size), np.arange(size)) % size
    angle = turns * (2.0 * math.pi / size)
    cosine, sine = np.cos(angle), np.sin(angle)
    return np.block([[cosine, sine], [-sine, cosine]])


def make_tables(outer, total):
    left, right = real_form(outer), real_form(128)
    turns = np.outer(np.arange(outer), np.arange(128)) % total
    angle = turns * (2.0 * math.pi / total)
    twist = np.stack([np.cos(angle), -np.sin(angle)]).astype(np.float32)
    return (
        split_table(left),
        split_table(left.T / total),
        split_table(right.T),
        split_table(right),
        twist,
    )


def halves(value):
    high = value.astype(bf16)
    return high, (value - high.astype(f32)).astype(bf16)


def mm(a, b):
    return jnp.dot(a, b, preferred_element_type=f32)


def left_dot(table, value):
    high, low = halves(value)
    return mm(table[0], high) + (mm(table[0], low) + mm(table[1], high))


def right_dot(value, table):
    high, low = halves(value)
    return mm(high, table[0]) + (mm(low, table[0]) + mm(high, table[1]))


def farthest_first(me, count):
    low, high = jnp.int32(0), jnp.int32(count - 1)
    peers = []
    for _ in range(count - 1):
        up = (high - me >= me - low).astype(jnp.int32)
        peers.append(up * high + (1 - up) * low)
        high, low = high - up, low + 1 - up
    return peers


def digits(shape, axis):
    return lax.broadcasted_iota(jnp.int32, shape, axis)


def one_hot(condition):
    return jnp.where(condition, 1.0, 0.0).astype(bf16)


def make_weights(sizes, pairs, mg, w1, w2, spread):
    Dt, Dm, B, Bl, ml, M, A, Al, As, Ak, J, total = sizes
    depth = J * 8
    group = max(1, 64 // M)
    step = group * M

    rows, cols = digits((step * 8, step), 0), digits((step * 8, step), 1)
    taller = one_hot(rows // 8 == cols)
    rows, cols = digits((2 * J, 3 * depth), 0), digits((2 * J, 3 * depth), 1)
    wider = one_hot((rows == cols % depth // 8 + jnp.where(cols < 2 * depth, 0, J)))
    kept = digits((step * 8, 3 * depth), 0) % 8 == digits((step * 8, 3 * depth), 1) % 8

    def block(p):
        return mg[p // ml, p % ml]

    columns = []
    for g in range(M // group):
        values = jnp.concatenate([block(g * group + i) for i in range(group)], axis=0)
        high, low = halves(values)
        both = jnp.concatenate([high.astype(f32), low.astype(f32)], axis=1).astype(bf16)
        tall = mm(taller, both).astype(bf16)
        wide = mm(tall, wider)
        w1[g * step * 8 : (g + 1) * step * 8, :] = jnp.where(kept, wide, 0.0).astype(bf16)
        columns.append((high, low))

    rows, cols = digits((depth, J), 0), digits((depth, J), 1)
    lifter = one_hot(rows // 8 == cols)

    def turned(values):
        return lax.dot_general(lifter, values, (((1,), (1,)), ((), ())), preferred_element_type=f32).astype(bf16)

    lifted = [[turned(part) for part in pair] for pair in columns]
    width = M * 8
    kept = digits((depth, 3 * width), 0) % 8 == digits((depth, 3 * width), 1) % 8
    rows, cols = digits((step, 3 * width), 0), digits((step, 3 * width), 1)

    def fill(n):
        total = jnp.zeros((depth, 3 * width), f32)
        for g, parts in enumerate(lifted):
            for which, part in enumerate(parts):
                inside = (cols >= 2 * width) if which else (cols < 2 * width)
                match = (rows // M + g * group == cols % width // 8) & (rows % M == n) & inside
                total = total + mm(part, one_hot(match))
        w2[pl.ds(pl.multiple_of(n * depth, depth), depth), :] = jnp.where(kept, total, 0.0).astype(bf16)

    if M <= 8:
        for n in range(M):
            fill(n)
    else:
        pl.loop(0, M)(fill)

    which = digits((8, 2 * depth), 1) // 8
    chosen = jnp.zeros((8, 2 * depth), jnp.int32)
    for side in range(2):
        for j in range(J):
            chosen = jnp.where(which == side * J + j, pairs[side, j], chosen)
    shape = (width, 2 * depth)
    match = (digits(shape, 0) // 8 == jnp.concatenate([chosen] * M, axis=0)) & (
        digits(shape, 0) % 8 == digits(shape, 1) % 8
    )
    spread[:, : 2 * depth] = one_hot(match)
    spread[:, 2 * depth :] = one_hot(match)


def kernel(
    sizes, kind, pairs, x, target, margin, beta_hbm,
    left_f_hbm, left_i_hbm, right_f_hbm, right_i_hbm, twist_hbm, out,
    left_f, left_i, right_f, right_i, twist, beta, phase_tab,
    rows_in, send_z, kb, t1, t2, mg, w1, w2, spread, pair_cols, coup, wanted, cots, push, push_cols, turn, move_cols,
    grads, rows_back, send_out,
    table_sem, own_sem, in_s, in_r, mg_ss, mg_r, t1_s, t1_r, t2_s, t2_r, kb_s, kb_r, gb_s, gb_r, out_s, out_r,
):
    Dt, Dm, B, Bl, ml, M, A, Al, As, Ak, J, total = sizes
    me_t = lax.axis_index("tm")
    me_m = lax.axis_index("mode")
    tm_peers = farthest_first(me_t, Dt)
    mode_peers = farthest_first(me_m, Dm)

    def remote(src, dst, send, recv, axis, peer):
        return pltpu.make_async_remote_copy(
            src_ref=src, dst_ref=dst, send_sem=send, recv_sem=recv, device_id={axis: peer}, device_id_type=MESH
        )

    barrier = pltpu.get_barrier_semaphore()
    for peer in tm_peers:
        pl.semaphore_signal(barrier, inc=1, device_id={"tm": peer}, device_id_type=MESH)
    for peer in mode_peers:
        pl.semaphore_signal(barrier, inc=1, device_id={"mode": peer}, device_id_type=MESH)
    pl.semaphore_wait(barrier, Dt + Dm - 2)

    sends = []
    owns = {}
    own_count = [0]

    def go(src, dst, send, recv, axis, peer):
        copy = remote(src, dst, send, recv, axis, peer)
        copy.start()
        sends.append(copy)

    def own(name, src, dst):
        copy = pltpu.make_async_copy(src, dst, own_sem.at[own_count[0]])
        own_count[0] += 1
        copy.start()
        owns[name] = copy

    def target_part(i, b):
        if (As * ml) % 8 == 0:
            return target.at[:, :, b, pl.ds(pl.multiple_of(i * (As * ml), 8), As * ml), :]
        return target.at[i, :, :, b]

    def target_first_leg(b):
        for peer in mode_peers:
            go(target_part(peer, b), t1[b].at[me_m], t1_s.at[b, peer], t1_r.at[b, me_m], "mode", peer)
        own(("t1", b), target_part(me_m, b), t1[b].at[me_m])

    def target_second_leg(b):
        owns[("t1", b)].wait()
        for peer in mode_peers:
            remote(target_part(0, b), t1[b].at[peer], t1_s.at[b, peer], t1_r.at[b, peer], "mode", peer).wait_recv()
        for peer in tm_peers:
            go(t1[b].at[:, :, peer], t2[b].at[me_t], t2_s.at[b, peer], t2_r.at[b, me_t], "tm", peer)
        own(("t2", b), t1[b].at[:, :, me_t], t2[b].at[me_t])

    for b in range(Bl):
        for peer in tm_peers:
            go(x.at[:, peer * Bl + b], rows_in.at[b, me_t], in_s.at[b, peer], in_r.at[b, me_t], "tm", peer)
        own(("in", b), x.at[:, me_t * Bl + b], rows_in.at[b, me_t])
    for peer in mode_peers:
        go(margin, mg.at[me_m], mg_ss.at[peer], mg_r.at[me_m], "mode", peer)
    own("mg", margin, mg.at[me_m])
    target_first_leg(0)
    table_copies = []
    for spot, (src, dst) in enumerate(
        ((left_f_hbm, left_f), (left_i_hbm, left_i), (right_f_hbm, right_f), (right_i_hbm, right_i), (twist_hbm, twist), (beta_hbm, beta))
    ):
        copy = pltpu.make_async_copy(src, dst, table_sem.at[spot])
        copy.start()
        table_copies.append(copy)

    for copy in table_copies:
        copy.wait()
    low_digit = lax.broadcasted_iota(jnp.int32, (A, 128), 0)
    high_digit = lax.broadcasted_iota(jnp.int32, (A, 128), 1)
    frequency = low_digit + A * high_digit
    signed = jnp.where(frequency < total // 2, frequency, frequency - total).astype(f32)
    omega = signed * (8.0 / total)
    for m in range(ml):
        phase = (
            beta[0, m, kind[0]] * omega
            + beta[1, m, kind[0]] * (omega * omega) / 2.0
            + beta[2, m, kind[0]] * (omega * omega * omega) / 6.0
        )
        phase_tab[0, m * A : (m + 1) * A, :] = jnp.cos(phase)
        phase_tab[1, m * A : (m + 1) * A, :] = jnp.sin(phase)
    def disperse(stacked, direction):
        spun = left_dot(left_f, stacked)
        tw_r, tw_i = twist[0], twist[1]
        blocks = []
        for m in range(ml):
            re = spun[:A, m * 128 : (m + 1) * 128]
            im = spun[A:, m * 128 : (m + 1) * 128]
            blocks.append(jnp.concatenate([re * tw_r - im * tw_i, re * tw_i + im * tw_r], axis=1))
        spectrum = right_dot(jnp.concatenate(blocks, axis=0), right_f)
        re, im = spectrum[:, :128], spectrum[:, 128:]
        cosine = phase_tab[0]
        sine = phase_tab[1] * direction
        turned = jnp.concatenate([re * cosine - im * sine, re * sine + im * cosine], axis=1)
        back = right_dot(turned, right_i)
        real_rows, imag_rows = [], []
        for m in range(ml):
            re = back[m * A : (m + 1) * A, :128]
            im = back[m * A : (m + 1) * A, 128:]
            real_rows.append(re * tw_r + im * tw_i)
            imag_rows.append(im * tw_r - re * tw_i)
        joined = jnp.concatenate(
            [jnp.concatenate(real_rows, axis=1), jnp.concatenate(imag_rows, axis=1)], axis=0
        )
        return left_dot(left_i, joined)

    owns["mg"].wait()
    for peer in mode_peers:
        remote(margin, mg.at[peer], mg_ss.at[peer], mg_r.at[peer], "mode", peer).wait_recv()
    make_weights(sizes, pairs, mg, w1, w2, spread)

    def kerr(b):
        field = kb[b]
        tiles = Ak // 8
        depth = J * 8

        for j in range(0, J, 2):
            made = []
            for s in range(2):
                first, second = pairs[0, j + s], pairs[1, j + s]
                ar, ai = field[first, 0], field[first, 1]
                br, bi = field[second, 0], field[second, 1]
                made.append((ar * br - ai * bi, ar * bi + ai * br))
            for q in range(tiles):
                for ri in range(2):
                    high, low = halves(
                        jnp.concatenate([made[s][ri][q * 8 : q * 8 + 8] for s in range(2)], axis=0)
                    )
                    cols = pl.ds((2 * q + ri) * 128, 128)
                    pair_cols[j * 8 : j * 8 + 16, cols] = high
                    pair_cols[depth + j * 8 : depth + j * 8 + 16, cols] = low
                    pair_cols[2 * depth + j * 8 : 2 * depth + j * 8 + 16, cols] = high
        for q in range(tiles):
            cols = pl.ds(q * 256, 256)
            coup[:, cols] = mm(w1[...], pair_cols[:, cols])

        @pl.loop(0, M)
        def _(p):
            owner, local = p // ml, lax.rem(p, ml)
            for ri in range(2):
                wanted[p, ri] = jnp.concatenate(
                    [t2[b][j, owner, ri, pl.ds(local, As, stride=ml), :] for j in range(Dt)], axis=0
                )

        @pl.loop(0, M // 2)
        def _(pp):
            for q in range(tiles):
                rows = pl.ds(q * 8, 8)
                pushed = []
                for s in range(2):
                    p = pp * 2 + s
                    kr = ki = jnp.zeros((8, 128), f32)
                    for n in range(M):
                        at = pl.ds(pl.multiple_of((p * M + n) * 8, 8), 8)
                        cr, ci = coup[at, q * 256 : q * 256 + 128], coup[at, q * 256 + 128 : q * 256 + 256]
                        ur, ui = field[n, 0, rows], field[n, 1, rows]
                        kr = kr + (cr * ur + ci * ui)
                        ki = ki + (ci * ur - cr * ui)
                    cr = 2.0 * (field[p, 0, rows] - kerr_scale * ki - wanted[p, 0, rows])
                    ci = 2.0 * (field[p, 1, rows] + kerr_scale * kr - wanted[p, 1, rows])
                    cots[p, 0, rows] = cr
                    cots[p, 1, rows] = ci
                    pushed.append((kerr_scale * ci, -kerr_scale * cr))
                    push[p, 0, rows] = pushed[s][0]
                    push[p, 1, rows] = pushed[s][1]
                for ri in range(2):
                    high, low = halves(jnp.concatenate([pushed[s][ri] for s in range(2)], axis=0))
                    cols = pl.ds((2 * q + ri) * 128, 128)
                    for part, value in enumerate((high, low, high)):
                        push_cols[pl.ds(pl.multiple_of(part * (M * 8) + pp * 16, 16), 16), cols] = value

        for q in range(tiles):
            cols = pl.ds(q * 256, 256)
            turn[:, cols] = mm(w2[...], push_cols[:, cols])

        @pl.loop(0, M)
        def _(n):
            for q in range(tiles):
                rows = pl.ds(q * 8, 8)
                gr, gi = cots[n, 0, rows], cots[n, 1, rows]
                for p in range(M):
                    at = pl.ds(pl.multiple_of((p * M + n) * 8, 8), 8)
                    cr, ci = coup[at, q * 256 : q * 256 + 128], coup[at, q * 256 + 128 : q * 256 + 256]
                    er, ei = push[p, 0, rows], push[p, 1, rows]
                    gr = gr + (er * cr + ei * ci)
                    gi = gi + (er * ci - ei * cr)
                cots[n, 0, rows] = gr
                cots[n, 1, rows] = gi

        @pl.loop(0, J // 2)
        def _(jj):
            for q in range(tiles):
                rows = pl.ds(q * 8, 8)
                moved = []
                for s in range(2):
                    j = jj * 2 + s
                    gr = gi = jnp.zeros((8, 128), f32)
                    for n in range(M):
                        at = pl.ds(pl.multiple_of((n * J + j) * 8, 8), 8)
                        tr, ti = turn[at, q * 256 : q * 256 + 128], turn[at, q * 256 + 128 : q * 256 + 256]
                        ur, ui = field[n, 0, rows], field[n, 1, rows]
                        gr = gr + (tr * ur - ti * ui)
                        gi = gi + (tr * ui + ti * ur)
                    for side in range(2):
                        other = pairs[1 - side, j]
                        vr, vi = field[other, 0, rows], field[other, 1, rows]
                        moved.append((side, (vr * gr + vi * gi, vr * gi - vi * gr)))
                for side in range(2):
                    for ri in range(2):
                        high, low = halves(
                            jnp.concatenate([value[ri] for which, value in moved if which == side], axis=0)
                        )
                        cols = pl.ds((2 * q + ri) * 128, 128)
                        at = side * depth + jj * 16
                        move_cols[pl.ds(pl.multiple_of(at, 16), 16), cols] = high
                        move_cols[pl.ds(pl.multiple_of(2 * depth + at, 16), 16), cols] = low

        for q in range(tiles):
            rows = pl.ds(q * 8, 8)
            back = mm(spread[...], move_cols[:, q * 256 : q * 256 + 256])
            for n in range(M):
                for ri in range(2):
                    grads[b, n, ri, rows] = (
                        cots[n, ri, rows] + back[n * 8 : n * 8 + 8, ri * 128 : ri * 128 + 128]
                    )

    for b in range(Bl):
        owns[("in", b)].wait()
        for peer in tm_peers:
            remote(x.at[:, b], rows_in.at[b, peer], in_s.at[b, peer], in_r.at[b, peer], "tm", peer).wait_recv()
        stacked = jnp.concatenate(
            [
                jnp.concatenate(
                    [rows_in[b, j, ri, pl.ds(m, Al, stride=ml), :] for ri in range(2) for j in range(Dt)], axis=0
                )
                for m in range(ml)
            ],
            axis=1,
        )
        result = disperse(stacked, 1.0)
        for i in range(Dm):
            for m in range(ml):
                for ri in range(2):
                    for j in range(Dt):
                        row = ri * A + j * Al + i * As
                        send_z[i, b, m, ri, j * As : (j + 1) * As, :] = result[row : row + As, m * 128 : (m + 1) * 128]
        for peer in mode_peers:
            go(send_z.at[peer, b], kb[b].at[pl.ds(me_m * ml, ml)], kb_s.at[b, peer], kb_r.at[b, me_m], "mode", peer)
        own(("kb", b), send_z.at[me_m, b], kb[b].at[pl.ds(me_m * ml, ml)])
        if b + 1 < Bl:
            target_first_leg(b + 1)
        if b == 0:
            target_second_leg(0)

    for b in range(Bl):
        owns[("kb", b)].wait()
        for peer in mode_peers:
            remote(
                send_z.at[0, b], kb[b].at[pl.ds(peer * ml, ml)], kb_s.at[b, peer], kb_r.at[b, peer], "mode", peer
            ).wait_recv()
        owns[("t2", b)].wait()
        for peer in tm_peers:
            remote(t1[b].at[:, :, 0], t2[b].at[peer], t2_s.at[b, peer], t2_r.at[b, peer], "tm", peer).wait_recv()

        kerr(b)

        for peer in mode_peers:
            go(grads.at[b, pl.ds(peer * ml, ml)], rows_back.at[b, me_m], gb_s.at[b, peer], gb_r.at[b, me_m], "mode", peer)
        if b + 1 < Bl:
            target_second_leg(b + 1)
        own(("gb", b), grads.at[b, pl.ds(me_m * ml, ml)], rows_back.at[b, me_m])

    for b in range(Bl):
        owns[("gb", b)].wait()
        for peer in mode_peers:
            remote(
                grads.at[b, pl.ds(0, ml)], rows_back.at[b, peer], gb_s.at[b, peer], gb_r.at[b, peer], "mode", peer
            ).wait_recv()
        stacked = jnp.concatenate(
            [
                jnp.concatenate(
                    [
                        rows_back[b, i, m, ri, j * As : (j + 1) * As, :]
                        for ri in range(2)
                        for j in range(Dt)
                        for i in range(Dm)
                    ],
                    axis=0,
                )
                for m in range(ml)
            ],
            axis=1,
        )
        result = disperse(stacked, -1.0)
        for j in range(Dt):
            for ri in range(2):
                for m in range(ml):
                    row = ri * A + j * Al
                    send_out[j, b, ri, pl.ds(m, Al, stride=ml), :] = result[row : row + Al, m * 128 : (m + 1) * 128]
        for peer in tm_peers:
            go(send_out.at[peer, b], out.at[:, me_t * Bl + b], out_s.at[b, peer], out_r.at[b, me_t], "tm", peer)
        own(("out", b), send_out.at[me_t, b], out.at[:, me_t * Bl + b])
    for b in range(Bl):
        owns[("out", b)].wait()
        for peer in tm_peers:
            remote(
                send_out.at[0, b], out.at[:, peer * Bl + b], out_s.at[b, peer], out_r.at[b, peer], "tm", peer
            ).wait_recv()
    for copy in sends:
        copy.wait_send()


def on_device(Dm, Dt, input_field, target_field, margin, pair_index, mode_beta, segment_kind):
    _, B, ml, Tl = input_field.shape
    M, J = margin.shape[1], margin.shape[2]
    total = Tl * Dt
    A = total // 128
    Al = Tl // 128
    Bl = B // Dt
    As = Al // Dm
    Ak = As * Dt
    def by_rows(values):
        return values.reshape(2, B, ml, Al, 128).transpose(0, 1, 3, 2, 4).reshape(2, B, Al * ml, 128)

    x = by_rows(input_field)
    target = by_rows(target_field).reshape(2, Dt, Bl, Al * ml, 128)
    if (As * ml) % 8:
        target = target.reshape(2, Dt, Bl, Dm, As * ml, 128).transpose(3, 0, 1, 2, 4, 5)
    tables = make_tables(A, total)
    sizes = (Dt, Dm, B, Bl, ml, M, A, Al, As, Ak, J, total)
    vm = lambda *shape: pltpu.VMEM(shape, f32)
    vb = lambda *shape: pltpu.VMEM(shape, bf16)
    dma = lambda *shape: pltpu.SemaphoreType.DMA(shape)
    anyspace = pl.BlockSpec(memory_space=pl.ANY)
    smem = pl.BlockSpec(memory_space=pltpu.SMEM)
    vmem = pl.BlockSpec(memory_space=pltpu.VMEM)
    out = pl.pallas_call(
        functools.partial(kernel, sizes),
        out_shape=jax.ShapeDtypeStruct((2, B, Al * ml, 128), f32),
        in_specs=[smem] * 2 + [anyspace, anyspace, vmem] + [anyspace] * 6,
        out_specs=vmem,
        scratch_shapes=[pltpu.VMEM(t.shape, bf16) for t in tables[:4]]
        + [
            vm(2, A, 128),
            pltpu.SMEM((3, ml, mode_beta.shape[0]), f32),
            vm(2, ml * A, 128),
            vm(Bl, Dt, 2, Al * ml, 128),
            vm(Dm, Bl, ml, 2, Ak, 128),
            [vm(M, 2, Ak, 128) for _ in range(Bl)],
            [vm(Dm, 2, Dt, As * ml, 128) for _ in range(Bl)],
            [vm(Dt, Dm, 2, As * ml, 128) for _ in range(Bl)],
            vm(Dm, ml, M, J),
            vb(M * M * 8, 3 * J * 8),
            vb(M * J * 8, 3 * M * 8),
            vb(M * 8, 4 * J * 8),
            vb(3 * J * 8, Ak * 32),
            vm(M * M * 8, Ak * 32),
            vm(M, 2, Ak, 128),
            vm(M, 2, Ak, 128),
            vm(M, 2, Ak, 128),
            vb(3 * M * 8, Ak * 32),
            vm(M * J * 8, Ak * 32),
            vb(4 * J * 8, Ak * 32),
            vm(Bl, M, 2, Ak, 128),
            vm(Bl, Dm, ml, 2, Ak, 128),
            vm(Dt, Bl, 2, Al * ml, 128),
            dma(6),
            dma(6 * Bl + 2),
            dma(Bl, Dt), dma(Bl, Dt),
            dma(Dm), dma(Dm),
            dma(Bl, Dm), dma(Bl, Dm),
            dma(Bl, Dt), dma(Bl, Dt),
            dma(Bl, Dm), dma(Bl, Dm),
            dma(Bl, Dm), dma(Bl, Dm),
            dma(Bl, Dt), dma(Bl, Dt),
        ],
        compiler_params=pltpu.CompilerParams(collective_id=0, has_side_effects=True, vmem_limit_bytes=62 * 1024 * 1024),
    )(segment_kind, pair_index.T, x, target, margin, mode_beta.transpose(2, 1, 0), *[jnp.asarray(t) for t in tables])
    return out.reshape(2, B, Al, ml, 128).transpose(0, 1, 3, 2, 4).reshape(2, B, ml, Tl)


def solution(mesh):
    return jax.shard_map(
        functools.partial(on_device, mesh.shape["mode"], mesh.shape["tm"]),
        mesh=mesh,
        in_specs=(
            P(None, "dp", "mode", "tm"),
            P(None, "dp", "mode", "tm"),
            P("mode", None, None),
            P(),
            P(None, "mode", None),
            P(),
        ),
        out_specs=P(None, "dp", "mode", "tm"),
        check_vma=False,
    )
```

```python
import functools
import math

import jax
import jax.numpy as jnp
import numpy as np
from jax import lax
from jax.experimental import pallas as pl
from jax.experimental.pallas import tpu as pltpu
from jax.sharding import PartitionSpec as P

kerr_scale = 0.1
MESH = pl.DeviceIdType.MESH
f32 = jnp.float32
bf16 = jnp.bfloat16


def split_table(table):
    high = table.astype(np.float32).astype(bf16)
    low = (table - high.astype(np.float64)).astype(np.float32).astype(bf16)
    return np.stack([np.asarray(high), np.asarray(low)])


def real_form(size):
    turns = np.outer(np.arange(size), np.arange(size)) % size
    angle = turns * (2.0 * math.pi / size)
    cosine, sine = np.cos(angle), np.sin(angle)
    return np.block([[cosine, sine], [-sine, cosine]])


def make_tables(outer, total):
    left, right = real_form(outer), real_form(128)
    turns = np.outer(np.arange(outer), np.arange(128)) % total
    angle = turns * (2.0 * math.pi / total)
    twist = np.stack([np.cos(angle), -np.sin(angle)]).astype(np.float32)
    return (
        split_table(left),
        split_table(left.T / total),
        split_table(right.T),
        split_table(right),
        twist,
    )


def halves(value):
    high = value.astype(bf16)
    return high, (value - high.astype(f32)).astype(bf16)


def mm(a, b):
    return jnp.dot(a, b, preferred_element_type=f32)


def left_dot(table, value):
    high, low = halves(value)
    return mm(table[0], high) + (mm(table[0], low) + mm(table[1], high))


def right_dot(value, table):
    high, low = halves(value)
    return mm(high, table[0]) + (mm(low, table[0]) + mm(high, table[1]))


def farthest_first(me, count):
    low, high = jnp.int32(0), jnp.int32(count - 1)
    peers = []
    for _ in range(count - 1):
        up = (high - me >= me - low).astype(jnp.int32)
        peers.append(up * high + (1 - up) * low)
        high, low = high - up, low + 1 - up
    return peers


def digits(shape, axis):
    return lax.broadcasted_iota(jnp.int32, shape, axis)


def one_hot(condition):
    return jnp.where(condition, 1.0, 0.0).astype(bf16)


def make_weights(sizes, pairs, mg, w1, w2, spread):
    Dt, Dm, B, Bl, ml, M, A, Al, As, Ak, J, total = sizes
    depth = J * 8
    group = max(1, 64 // M)
    step = group * M

    rows, cols = digits((step * 8, step), 0), digits((step * 8, step), 1)
    taller = one_hot(rows // 8 == cols)
    rows, cols = digits((2 * J, 3 * depth), 0), digits((2 * J, 3 * depth), 1)
    wider = one_hot((rows == cols % depth // 8 + jnp.where(cols < 2 * depth, 0, J)))
    kept = digits((step * 8, 3 * depth), 0) % 8 == digits((step * 8, 3 * depth), 1) % 8

    def block(p):
        return mg[p // ml, p % ml]

    columns = []
    for g in range(M // group):
        values = jnp.concatenate([block(g * group + i) for i in range(group)], axis=0)
        high, low = halves(values)
        both = jnp.concatenate([high.astype(f32), low.astype(f32)], axis=1).astype(bf16)
        tall = mm(taller, both).astype(bf16)
        wide = mm(tall, wider)
        w1[g * step * 8 : (g + 1) * step * 8, :] = jnp.where(kept, wide, 0.0).astype(bf16)
        columns.append((high, low))

    rows, cols = digits((depth, J), 0), digits((depth, J), 1)
    lifter = one_hot(rows // 8 == cols)

    def turned(values):
        return lax.dot_general(lifter, values, (((1,), (1,)), ((), ())), preferred_element_type=f32).astype(bf16)

    lifted = [[turned(part) for part in pair] for pair in columns]
    width = M * 8
    kept = digits((depth, 3 * width), 0) % 8 == digits((depth, 3 * width), 1) % 8
    rows, cols = digits((step, 3 * width), 0), digits((step, 3 * width), 1)

    def fill(n):
        total = jnp.zeros((depth, 3 * width), f32)
        for g, parts in enumerate(lifted):
            for which, part in enumerate(parts):
                inside = (cols >= 2 * width) if which else (cols < 2 * width)
                match = (rows // M + g * group == cols % width // 8) & (rows % M == n) & inside
                total = total + mm(part, one_hot(match))
        w2[pl.ds(pl.multiple_of(n * depth, depth), depth), :] = jnp.where(kept, total, 0.0).astype(bf16)

    if M <= 8:
        for n in range(M):
            fill(n)
    else:
        pl.loop(0, M)(fill)

    which = digits((8, 2 * depth), 1) // 8
    chosen = jnp.zeros((8, 2 * depth), jnp.int32)
    for side in range(2):
        for j in range(J):
            chosen = jnp.where(which == side * J + j, pairs[side, j], chosen)
    shape = (width, 2 * depth)
    match = (digits(shape, 0) // 8 == jnp.concatenate([chosen] * M, axis=0)) & (
        digits(shape, 0) % 8 == digits(shape, 1) % 8
    )
    spread[:, : 2 * depth] = one_hot(match)
    spread[:, 2 * depth :] = one_hot(match)


def kernel(
    sizes, kind, pairs, x, target, margin, beta_hbm,
    left_f_hbm, left_i_hbm, right_f_hbm, right_i_hbm, twist_hbm, out,
    x_near, target_near, left_f, left_i, right_f, right_i, twist, beta, phase_tab,
    rows_in, send_z, kb, t1, t2, mg, w1, w2, spread, pair_cols, coup, wanted, cots, push, push_cols, turn, move_cols,
    grads, rows_back, send_out,
    near_sem, table_sem, own_sem, in_s, in_r, mg_ss, mg_r, t1_s, t1_r, t2_s, t2_r, kb_s, kb_r, gb_s, gb_r, out_s, out_r,
):
    Dt, Dm, B, Bl, ml, M, A, Al, As, Ak, J, total = sizes
    me_t = lax.axis_index("tm")
    me_m = lax.axis_index("mode")
    tm_peers = farthest_first(me_t, Dt)
    mode_peers = farthest_first(me_m, Dm)

    def remote(src, dst, send, recv, axis, peer):
        return pltpu.make_async_remote_copy(
            src_ref=src, dst_ref=dst, send_sem=send, recv_sem=recv, device_id={axis: peer}, device_id_type=MESH
        )

    staged = [pltpu.make_async_copy(x, x_near, near_sem.at[0]), pltpu.make_async_copy(target, target_near, near_sem.at[1])]
    for copy in staged:
        copy.start()

    barrier = pltpu.get_barrier_semaphore()
    for peer in tm_peers:
        pl.semaphore_signal(barrier, inc=1, device_id={"tm": peer}, device_id_type=MESH)
    for peer in mode_peers:
        pl.semaphore_signal(barrier, inc=1, device_id={"mode": peer}, device_id_type=MESH)
    pl.semaphore_wait(barrier, Dt + Dm - 2)

    sends = []
    owns = {}
    own_count = [0]

    def go(src, dst, send, recv, axis, peer):
        copy = remote(src, dst, send, recv, axis, peer)
        copy.start()
        sends.append(copy)

    def own(name, src, dst):
        copy = pltpu.make_async_copy(src, dst, own_sem.at[own_count[0]])
        own_count[0] += 1
        copy.start()
        owns[name] = copy

    def target_part(i, b):
        if (As * ml) % 8 == 0:
            return target_near.at[:, :, b, pl.ds(pl.multiple_of(i * (As * ml), 8), As * ml), :]
        return target_near.at[i, :, :, b]

    def target_first_leg(b):
        for peer in mode_peers:
            go(target_part(peer, b), t1[b].at[me_m], t1_s.at[b, peer], t1_r.at[b, me_m], "mode", peer)
        own(("t1", b), target_part(me_m, b), t1[b].at[me_m])

    def target_second_leg(b):
        owns[("t1", b)].wait()
        for peer in mode_peers:
            remote(target_part(0, b), t1[b].at[peer], t1_s.at[b, peer], t1_r.at[b, peer], "mode", peer).wait_recv()
        for peer in tm_peers:
            go(t1[b].at[:, :, peer], t2[b].at[me_t], t2_s.at[b, peer], t2_r.at[b, me_t], "tm", peer)
        own(("t2", b), t1[b].at[:, :, me_t], t2[b].at[me_t])

    staged[0].wait()
    for b in range(Bl):
        for peer in tm_peers:
            go(x_near.at[:, peer * Bl + b], rows_in.at[b, me_t], in_s.at[b, peer], in_r.at[b, me_t], "tm", peer)
        own(("in", b), x_near.at[:, me_t * Bl + b], rows_in.at[b, me_t])
    for peer in mode_peers:
        go(margin, mg.at[me_m], mg_ss.at[peer], mg_r.at[me_m], "mode", peer)
    own("mg", margin, mg.at[me_m])
    staged[1].wait()
    for b in range(Bl):
        target_first_leg(b)
    table_copies = []
    for spot, (src, dst) in enumerate(
        ((left_f_hbm, left_f), (left_i_hbm, left_i), (right_f_hbm, right_f), (right_i_hbm, right_i), (twist_hbm, twist), (beta_hbm, beta))
    ):
        copy = pltpu.make_async_copy(src, dst, table_sem.at[spot])
        copy.start()
        table_copies.append(copy)

    for copy in table_copies:
        copy.wait()
    low_digit = lax.broadcasted_iota(jnp.int32, (A, 128), 0)
    high_digit = lax.broadcasted_iota(jnp.int32, (A, 128), 1)
    frequency = low_digit + A * high_digit
    signed = jnp.where(frequency < total // 2, frequency, frequency - total).astype(f32)
    omega = signed * (8.0 / total)
    for m in range(ml):
        phase = (
            beta[0, m, kind[0]] * omega
            + beta[1, m, kind[0]] * (omega * omega) / 2.0
            + beta[2, m, kind[0]] * (omega * omega * omega) / 6.0
        )
        phase_tab[0, m * A : (m + 1) * A, :] = jnp.cos(phase)
        phase_tab[1, m * A : (m + 1) * A, :] = jnp.sin(phase)
    def disperse(stacked, direction, modes):
        spun = left_dot(left_f, stacked)
        tw_r, tw_i = twist[0], twist[1]
        blocks = []
        for m in range(len(modes)):
            re = spun[:A, m * 128 : (m + 1) * 128]
            im = spun[A:, m * 128 : (m + 1) * 128]
            blocks.append(jnp.concatenate([re * tw_r - im * tw_i, re * tw_i + im * tw_r], axis=1))
        spectrum = right_dot(jnp.concatenate(blocks, axis=0), right_f)
        re, im = spectrum[:, :128], spectrum[:, 128:]
        cosine, sine = (
            jnp.concatenate([phase_tab[part, m * A : (m + 1) * A, :] for m in modes], axis=0) for part in range(2)
        )
        sine = sine * direction
        turned = jnp.concatenate([re * cosine - im * sine, re * sine + im * cosine], axis=1)
        back = right_dot(turned, right_i)
        real_rows, imag_rows = [], []
        for m in range(len(modes)):
            re = back[m * A : (m + 1) * A, :128]
            im = back[m * A : (m + 1) * A, 128:]
            real_rows.append(re * tw_r + im * tw_i)
            imag_rows.append(im * tw_r - re * tw_i)
        joined = jnp.concatenate(
            [jnp.concatenate(real_rows, axis=1), jnp.concatenate(imag_rows, axis=1)], axis=0
        )
        return left_dot(left_i, joined)

    def kerr(b):
        field = kb[b]
        tiles = Ak // 8
        depth = J * 8

        for j in range(0, J, 2):
            made = []
            for s in range(2):
                first, second = pairs[0, j + s], pairs[1, j + s]
                ar, ai = field[first, 0], field[first, 1]
                br, bi = field[second, 0], field[second, 1]
                made.append((ar * br - ai * bi, ar * bi + ai * br))
            for q in range(tiles):
                for ri in range(2):
                    high, low = halves(
                        jnp.concatenate([made[s][ri][q * 8 : q * 8 + 8] for s in range(2)], axis=0)
                    )
                    cols = pl.ds((2 * q + ri) * 128, 128)
                    pair_cols[j * 8 : j * 8 + 16, cols] = high
                    pair_cols[depth + j * 8 : depth + j * 8 + 16, cols] = low
                    pair_cols[2 * depth + j * 8 : 2 * depth + j * 8 + 16, cols] = high
        for q in range(tiles):
            cols = pl.ds(q * 256, 256)
            coup[:, cols] = mm(w1[...], pair_cols[:, cols])

        @pl.loop(0, M)
        def _(p):
            owner, local = p // ml, lax.rem(p, ml)
            for ri in range(2):
                wanted[p, ri] = jnp.concatenate(
                    [t2[b][j, owner, ri, pl.ds(local, As, stride=ml), :] for j in range(Dt)], axis=0
                )

        @pl.loop(0, M // 2)
        def _(pp):
            for q in range(tiles):
                rows = pl.ds(q * 8, 8)
                pushed = []
                for s in range(2):
                    p = pp * 2 + s
                    kr = ki = jnp.zeros((8, 128), f32)
                    for n in range(M):
                        at = pl.ds(pl.multiple_of((p * M + n) * 8, 8), 8)
                        cr, ci = coup[at, q * 256 : q * 256 + 128], coup[at, q * 256 + 128 : q * 256 + 256]
                        ur, ui = field[n, 0, rows], field[n, 1, rows]
                        kr = kr + (cr * ur + ci * ui)
                        ki = ki + (ci * ur - cr * ui)
                    cr = 2.0 * (field[p, 0, rows] - kerr_scale * ki - wanted[p, 0, rows])
                    ci = 2.0 * (field[p, 1, rows] + kerr_scale * kr - wanted[p, 1, rows])
                    cots[p, 0, rows] = cr
                    cots[p, 1, rows] = ci
                    pushed.append((kerr_scale * ci, -kerr_scale * cr))
                    push[p, 0, rows] = pushed[s][0]
                    push[p, 1, rows] = pushed[s][1]
                for ri in range(2):
                    high, low = halves(jnp.concatenate([pushed[s][ri] for s in range(2)], axis=0))
                    cols = pl.ds((2 * q + ri) * 128, 128)
                    for part, value in enumerate((high, low, high)):
                        push_cols[pl.ds(pl.multiple_of(part * (M * 8) + pp * 16, 16), 16), cols] = value

        for q in range(tiles):
            cols = pl.ds(q * 256, 256)
            turn[:, cols] = mm(w2[...], push_cols[:, cols])

        @pl.loop(0, M)
        def _(n):
            for q in range(tiles):
                rows = pl.ds(q * 8, 8)
                gr, gi = cots[n, 0, rows], cots[n, 1, rows]
                for p in range(M):
                    at = pl.ds(pl.multiple_of((p * M + n) * 8, 8), 8)
                    cr, ci = coup[at, q * 256 : q * 256 + 128], coup[at, q * 256 + 128 : q * 256 + 256]
                    er, ei = push[p, 0, rows], push[p, 1, rows]
                    gr = gr + (er * cr + ei * ci)
                    gi = gi + (er * ci - ei * cr)
                cots[n, 0, rows] = gr
                cots[n, 1, rows] = gi

        @pl.loop(0, J // 2)
        def _(jj):
            for q in range(tiles):
                rows = pl.ds(q * 8, 8)
                moved = []
                for s in range(2):
                    j = jj * 2 + s
                    gr = gi = jnp.zeros((8, 128), f32)
                    for n in range(M):
                        at = pl.ds(pl.multiple_of((n * J + j) * 8, 8), 8)
                        tr, ti = turn[at, q * 256 : q * 256 + 128], turn[at, q * 256 + 128 : q * 256 + 256]
                        ur, ui = field[n, 0, rows], field[n, 1, rows]
                        gr = gr + (tr * ur - ti * ui)
                        gi = gi + (tr * ui + ti * ur)
                    for side in range(2):
                        other = pairs[1 - side, j]
                        vr, vi = field[other, 0, rows], field[other, 1, rows]
                        moved.append((side, (vr * gr + vi * gi, vr * gi - vi * gr)))
                for side in range(2):
                    for ri in range(2):
                        high, low = halves(
                            jnp.concatenate([value[ri] for which, value in moved if which == side], axis=0)
                        )
                        cols = pl.ds((2 * q + ri) * 128, 128)
                        at = side * depth + jj * 16
                        move_cols[pl.ds(pl.multiple_of(at, 16), 16), cols] = high
                        move_cols[pl.ds(pl.multiple_of(2 * depth + at, 16), 16), cols] = low

        for q in range(tiles):
            rows = pl.ds(q * 8, 8)
            back = mm(spread[...], move_cols[:, q * 256 : q * 256 + 256])
            for n in range(M):
                for ri in range(2):
                    grads[b, n, ri, rows] = (
                        cots[n, ri, rows] + back[n * 8 : n * 8 + 8, ri * 128 : ri * 128 + 128]
                    )

    for b in range(Bl):
        owns[("in", b)].wait()
        for peer in tm_peers:
            remote(x_near.at[:, b], rows_in.at[b, peer], in_s.at[b, peer], in_r.at[b, peer], "tm", peer).wait_recv()
        stacked = jnp.concatenate(
            [
                jnp.concatenate(
                    [rows_in[b, j, ri, pl.ds(m, Al, stride=ml), :] for ri in range(2) for j in range(Dt)], axis=0
                )
                for m in range(ml)
            ],
            axis=1,
        )
        result = disperse(stacked, 1.0, range(ml))
        for i in range(Dm):
            for m in range(ml):
                for ri in range(2):
                    for j in range(Dt):
                        row = ri * A + j * Al + i * As
                        send_z[i, b, m, ri, j * As : (j + 1) * As, :] = result[row : row + As, m * 128 : (m + 1) * 128]
        for peer in mode_peers:
            go(send_z.at[peer, b], kb[b].at[pl.ds(me_m * ml, ml)], kb_s.at[b, peer], kb_r.at[b, me_m], "mode", peer)
        own(("kb", b), send_z.at[me_m, b], kb[b].at[pl.ds(me_m * ml, ml)])
        if b == 0:
            target_second_leg(0)

    owns["mg"].wait()
    for peer in mode_peers:
        remote(margin, mg.at[peer], mg_ss.at[peer], mg_r.at[peer], "mode", peer).wait_recv()
    make_weights(sizes, pairs, mg, w1, w2, spread)
    for b in range(1, Bl):
        target_second_leg(b)

    for b in range(Bl):
        owns[("kb", b)].wait()
        for peer in mode_peers:
            remote(
                send_z.at[0, b], kb[b].at[pl.ds(peer * ml, ml)], kb_s.at[b, peer], kb_r.at[b, peer], "mode", peer
            ).wait_recv()
        owns[("t2", b)].wait()
        for peer in tm_peers:
            remote(t1[b].at[:, :, 0], t2[b].at[peer], t2_s.at[b, peer], t2_r.at[b, peer], "tm", peer).wait_recv()

        kerr(b)

        for m in range(ml):
            for peer in mode_peers:
                go(
                    grads.at[b, peer * ml + m], rows_back.at[b, m, me_m],
                    gb_s.at[b, m, peer], gb_r.at[b, m, me_m], "mode", peer,
                )
            own(("gb", b, m), grads.at[b, me_m * ml + m], rows_back.at[b, m, me_m])

    for b in range(Bl):
        for m in range(ml):
            owns[("gb", b, m)].wait()
            for peer in mode_peers:
                remote(
                    grads.at[b, m], rows_back.at[b, m, peer], gb_s.at[b, m, peer], gb_r.at[b, m, peer], "mode", peer
                ).wait_recv()
            stacked = jnp.concatenate(
                [
                    rows_back[b, m, i, ri, j * As : (j + 1) * As, :]
                    for ri in range(2)
                    for j in range(Dt)
                    for i in range(Dm)
                ],
                axis=0,
            )
            result = disperse(stacked, -1.0, [m])
            for j in range(Dt):
                for ri in range(2):
                    row = ri * A + j * Al
                    send_out[j, b, m, ri] = result[row : row + Al, :]
            for peer in tm_peers:
                go(
                    send_out.at[peer, b, m], out.at[:, me_t * Bl + b, m],
                    out_s.at[b, m, peer], out_r.at[b, m, me_t], "tm", peer,
                )
            own(("out", b, m), send_out.at[me_t, b, m], out.at[:, me_t * Bl + b, m])
    for b in range(Bl):
        for m in range(ml):
            owns[("out", b, m)].wait()
            for peer in tm_peers:
                remote(
                    send_out.at[0, b, m], out.at[:, peer * Bl + b, m],
                    out_s.at[b, m, peer], out_r.at[b, m, peer], "tm", peer,
                ).wait_recv()
    for copy in sends:
        copy.wait_send()


def finish(gathered, out, woven, sem):
    _, B, ml, Al, _ = gathered.shape
    copies = []
    for b in range(B):
        for ri in range(2):
            for m in range(ml):
                woven[ri, b, pl.ds(m, Al, stride=ml), :] = gathered[ri, b, m]
        copy = pltpu.make_async_copy(woven.at[:, b], out.at[:, b], sem.at[b])
        copy.start()
        copies.append(copy)
    for copy in copies:
        copy.wait()


def on_device(Dm, Dt, input_field, target_field, margin, pair_index, mode_beta, segment_kind):
    _, B, ml, Tl = input_field.shape
    M, J = margin.shape[1], margin.shape[2]
    total = Tl * Dt
    A = total // 128
    Al = Tl // 128
    Bl = B // Dt
    As = Al // Dm
    Ak = As * Dt
    def by_rows(values):
        return values.reshape(2, B, ml, Al, 128).transpose(0, 1, 3, 2, 4).reshape(2, B, Al * ml, 128)

    x = by_rows(input_field)
    target = by_rows(target_field).reshape(2, Dt, Bl, Al * ml, 128)
    if (As * ml) % 8:
        target = target.reshape(2, Dt, Bl, Dm, As * ml, 128).transpose(3, 0, 1, 2, 4, 5)
    tables = make_tables(A, total)
    sizes = (Dt, Dm, B, Bl, ml, M, A, Al, As, Ak, J, total)
    vm = lambda *shape: pltpu.VMEM(shape, f32)
    vb = lambda *shape: pltpu.VMEM(shape, bf16)
    dma = lambda *shape: pltpu.SemaphoreType.DMA(shape)
    anyspace = pl.BlockSpec(memory_space=pl.ANY)
    smem = pl.BlockSpec(memory_space=pltpu.SMEM)
    vmem = pl.BlockSpec(memory_space=pltpu.VMEM)
    gathered = pl.pallas_call(
        functools.partial(kernel, sizes),
        out_shape=pltpu.VMEM((2, B, ml, Al, 128), f32),
        in_specs=[smem] * 2 + [anyspace, anyspace, vmem] + [anyspace] * 6,
        out_specs=vmem,
        scratch_shapes=[vm(*x.shape), vm(*target.shape)]
        + [pltpu.VMEM(t.shape, bf16) for t in tables[:4]]
        + [
            vm(2, A, 128),
            pltpu.SMEM((3, ml, mode_beta.shape[0]), f32),
            vm(2, ml * A, 128),
            vm(Bl, Dt, 2, Al * ml, 128),
            vm(Dm, Bl, ml, 2, Ak, 128),
            [vm(M, 2, Ak, 128) for _ in range(Bl)],
            [vm(Dm, 2, Dt, As * ml, 128) for _ in range(Bl)],
            [vm(Dt, Dm, 2, As * ml, 128) for _ in range(Bl)],
            vm(Dm, ml, M, J),
            vb(M * M * 8, 3 * J * 8),
            vb(M * J * 8, 3 * M * 8),
            vb(M * 8, 4 * J * 8),
            vb(3 * J * 8, Ak * 32),
            vm(M * M * 8, Ak * 32),
            vm(M, 2, Ak, 128),
            vm(M, 2, Ak, 128),
            vm(M, 2, Ak, 128),
            vb(3 * M * 8, Ak * 32),
            vm(M * J * 8, Ak * 32),
            vb(4 * J * 8, Ak * 32),
            vm(Bl, M, 2, Ak, 128),
            vm(Bl, ml, Dm, 2, Ak, 128),
            vm(Dt, Bl, ml, 2, Al, 128),
            dma(2),
            dma(6),
            dma((4 + 2 * ml) * Bl + 1),
            dma(Bl, Dt), dma(Bl, Dt),
            dma(Dm), dma(Dm),
            dma(Bl, Dm), dma(Bl, Dm),
            dma(Bl, Dt), dma(Bl, Dt),
            dma(Bl, Dm), dma(Bl, Dm),
            dma(Bl, ml, Dm), dma(Bl, ml, Dm),
            dma(Bl, ml, Dt), dma(Bl, ml, Dt),
        ],
        compiler_params=pltpu.CompilerParams(collective_id=0, has_side_effects=True, vmem_limit_bytes=62 * 1024 * 1024),
    )(segment_kind, pair_index.T, x, target, margin, mode_beta.transpose(2, 1, 0), *[jnp.asarray(t) for t in tables])
    out = pl.pallas_call(
        finish,
        out_shape=jax.ShapeDtypeStruct((2, B, Al * ml, 128), f32),
        in_specs=[vmem],
        out_specs=anyspace,
        scratch_shapes=[vm(2, B, Al * ml, 128), dma(B)],
    )(pltpu.with_memory_space_constraint(gathered, pltpu.VMEM))
    return out.reshape(2, B, Al, ml, 128).transpose(0, 1, 3, 2, 4).reshape(2, B, ml, Tl)


def solution(mesh):
    return jax.shard_map(
        functools.partial(on_device, mesh.shape["mode"], mesh.shape["tm"]),
        mesh=mesh,
        in_specs=(
            P(None, "dp", "mode", "tm"),
            P(None, "dp", "mode", "tm"),
            P("mode", None, None),
            P(),
            P(None, "mode", None),
            P(),
        ),
        out_specs=P(None, "dp", "mode", "tm"),
        check_vma=False,
    )
```

```python
import functools
import math

import jax
import jax.numpy as jnp
import numpy as np
from jax import lax
from jax.experimental import pallas as pl
from jax.experimental.pallas import tpu as pltpu
from jax.sharding import PartitionSpec as P

kerr_scale = 0.1
MESH = pl.DeviceIdType.MESH
f32 = jnp.float32
bf16 = jnp.bfloat16


def split_table(table):
    high = table.astype(np.float32).astype(bf16)
    low = (table - high.astype(np.float64)).astype(np.float32).astype(bf16)
    return np.stack([np.asarray(high), np.asarray(low)])


def real_form(size):
    turns = np.outer(np.arange(size), np.arange(size)) % size
    angle = turns * (2.0 * math.pi / size)
    cosine, sine = np.cos(angle), np.sin(angle)
    return np.block([[cosine, sine], [-sine, cosine]])


def make_tables(outer, total):
    left, right = real_form(outer), real_form(128)
    turns = np.outer(np.arange(outer), np.arange(128)) % total
    angle = turns * (2.0 * math.pi / total)
    twist = np.stack([np.cos(angle), -np.sin(angle)]).astype(np.float32)
    return (
        split_table(left),
        split_table(left.T / total),
        split_table(right.T),
        split_table(right),
        twist,
    )


def halves(value):
    high = value.astype(bf16)
    return high, (value - high.astype(f32)).astype(bf16)


def mm(a, b):
    return jnp.dot(a, b, preferred_element_type=f32)


def left_dot(table, value):
    high, low = halves(value)
    return mm(table[0], high) + (mm(table[0], low) + mm(table[1], high))


def right_dot(value, table):
    high, low = halves(value)
    return mm(high, table[0]) + (mm(low, table[0]) + mm(high, table[1]))


def farthest_first(me, count):
    low, high = jnp.int32(0), jnp.int32(count - 1)
    peers = []
    for _ in range(count - 1):
        up = (high - me >= me - low).astype(jnp.int32)
        peers.append(up * high + (1 - up) * low)
        high, low = high - up, low + 1 - up
    return peers


def digits(shape, axis):
    return lax.broadcasted_iota(jnp.int32, shape, axis)


def one_hot(condition):
    return jnp.where(condition, 1.0, 0.0).astype(bf16)


def make_weights(sizes, pairs, mg, w1, w2, spread):
    Dt, Dm, B, Bl, ml, M, A, Al, As, Ak, J, total = sizes
    depth = J * 8
    group = max(1, 64 // M)
    step = group * M

    rows, cols = digits((step * 8, step), 0), digits((step * 8, step), 1)
    taller = one_hot(rows // 8 == cols)
    rows, cols = digits((2 * J, 3 * depth), 0), digits((2 * J, 3 * depth), 1)
    wider = one_hot((rows == cols % depth // 8 + jnp.where(cols < 2 * depth, 0, J)))
    kept = digits((step * 8, 3 * depth), 0) % 8 == digits((step * 8, 3 * depth), 1) % 8

    def block(p):
        return mg[p // ml, p % ml]

    columns = []
    for g in range(M // group):
        values = jnp.concatenate([block(g * group + i) for i in range(group)], axis=0)
        high, low = halves(values)
        both = jnp.concatenate([high.astype(f32), low.astype(f32)], axis=1).astype(bf16)
        tall = mm(taller, both).astype(bf16)
        wide = mm(tall, wider)
        w1[g * step * 8 : (g + 1) * step * 8, :] = jnp.where(kept, wide, 0.0).astype(bf16)
        columns.append((high, low))

    rows, cols = digits((depth, J), 0), digits((depth, J), 1)
    lifter = one_hot(rows // 8 == cols)

    def turned(values):
        return lax.dot_general(lifter, values, (((1,), (1,)), ((), ())), preferred_element_type=f32).astype(bf16)

    lifted = [[turned(part) for part in pair] for pair in columns]
    width = M * 8
    kept = digits((depth, 3 * width), 0) % 8 == digits((depth, 3 * width), 1) % 8
    rows, cols = digits((step, 3 * width), 0), digits((step, 3 * width), 1)

    def fill(n):
        total = jnp.zeros((depth, 3 * width), f32)
        for g, parts in enumerate(lifted):
            for which, part in enumerate(parts):
                inside = (cols >= 2 * width) if which else (cols < 2 * width)
                match = (rows // M + g * group == cols % width // 8) & (rows % M == n) & inside
                total = total + mm(part, one_hot(match))
        w2[pl.ds(pl.multiple_of(n * depth, depth), depth), :] = jnp.where(kept, total, 0.0).astype(bf16)

    if M <= 8:
        for n in range(M):
            fill(n)
    else:
        pl.loop(0, M)(fill)

    which = digits((8, 2 * depth), 1) // 8
    chosen = jnp.zeros((8, 2 * depth), jnp.int32)
    for side in range(2):
        for j in range(J):
            chosen = jnp.where(which == side * J + j, pairs[side, j], chosen)
    shape = (width, 2 * depth)
    match = (digits(shape, 0) // 8 == jnp.concatenate([chosen] * M, axis=0)) & (
        digits(shape, 0) % 8 == digits(shape, 1) % 8
    )
    spread[:, : 2 * depth] = one_hot(match)
    spread[:, 2 * depth :] = one_hot(match)


def kernel(
    sizes, kind_hbm, pairs_hbm, x, target, margin_hbm, beta_hbm,
    left_f_hbm, left_i_hbm, right_f_hbm, right_i_hbm, twist_hbm, out,
    x_near, target_near, kind, pairs, margin, left_f, left_i, right_f, right_i, twist, beta, phase_tab,
    rows_in, send_z, kb, t1, t2, mg, w1, w2, spread, pair_cols, coup, wanted, cots, push, push_cols, turn, move_cols,
    grads, rows_back, send_out,
    near_sem, table_sem, own_sem, in_s, in_r, mg_ss, mg_r, t1_s, t1_r, t2_s, t2_r, kb_s, kb_r, gb_s, gb_r, out_s, out_r,
):
    Dt, Dm, B, Bl, ml, M, A, Al, As, Ak, J, total = sizes
    parts = 2 if Ak % 16 == 0 else 1
    Hk = Ak // parts
    me_t = lax.axis_index("tm")
    me_m = lax.axis_index("mode")
    tm_peers = farthest_first(me_t, Dt)
    mode_peers = farthest_first(me_m, Dm)

    def remote(src, dst, send, recv, axis, peer):
        return pltpu.make_async_remote_copy(
            src_ref=src, dst_ref=dst, send_sem=send, recv_sem=recv, device_id={axis: peer}, device_id_type=MESH
        )

    barrier = pltpu.get_barrier_semaphore()
    for peer in mode_peers:
        pl.semaphore_signal(barrier, inc=1, device_id={"mode": peer}, device_id_type=MESH)
    for peer in tm_peers:
        pl.semaphore_signal(barrier, inc=1, device_id={"tm": peer}, device_id_type=MESH)
    staged = []
    for spot, (src, dst) in enumerate(
        ((margin_hbm, margin), (target, target_near), (x, x_near), (kind_hbm, kind), (pairs_hbm, pairs))
    ):
        staged.append(pltpu.make_async_copy(src, dst, near_sem.at[spot]))
        staged[-1].start()
    pl.semaphore_wait(barrier, Dt + Dm - 2)

    sends = []
    owns = {}
    own_count = [0]

    def go(src, dst, send, recv, axis, peer):
        copy = remote(src, dst, send, recv, axis, peer)
        copy.start()
        sends.append(copy)

    def own(name, src, dst):
        copy = pltpu.make_async_copy(src, dst, own_sem.at[own_count[0]])
        own_count[0] += 1
        copy.start()
        owns[name] = copy

    def target_part(i, b):
        if (As * ml) % 8 == 0:
            return target_near.at[:, :, b, pl.ds(pl.multiple_of(i * (As * ml), 8), As * ml), :]
        return target_near.at[i, :, :, b]

    def target_first_leg(b):
        for peer in mode_peers:
            go(target_part(peer, b), t1[b].at[me_m], t1_s.at[b, peer], t1_r.at[b, me_m], "mode", peer)
        own(("t1", b), target_part(me_m, b), t1[b].at[me_m])

    def target_second_leg(b):
        owns[("t1", b)].wait()
        for peer in mode_peers:
            remote(target_part(0, b), t1[b].at[peer], t1_s.at[b, peer], t1_r.at[b, peer], "mode", peer).wait_recv()
        for peer in tm_peers:
            go(t1[b].at[:, :, peer], t2[b].at[me_t], t2_s.at[b, peer], t2_r.at[b, me_t], "tm", peer)
        own(("t2", b), t1[b].at[:, :, me_t], t2[b].at[me_t])

    staged[0].wait()
    for peer in mode_peers:
        go(margin, mg.at[me_m], mg_ss.at[peer], mg_r.at[me_m], "mode", peer)
    own("mg", margin, mg.at[me_m])
    staged[1].wait()
    target_first_leg(0)
    staged[2].wait()
    for b in range(Bl):
        for peer in tm_peers:
            go(x_near.at[:, peer * Bl + b], rows_in.at[b, me_t], in_s.at[b, peer], in_r.at[b, me_t], "tm", peer)
        own(("in", b), x_near.at[:, me_t * Bl + b], rows_in.at[b, me_t])
    for b in range(1, Bl):
        target_first_leg(b)
    for copy in staged[3:]:
        copy.wait()
    table_copies = []
    for spot, (src, dst) in enumerate(
        ((left_f_hbm, left_f), (left_i_hbm, left_i), (right_f_hbm, right_f), (right_i_hbm, right_i), (twist_hbm, twist), (beta_hbm, beta))
    ):
        copy = pltpu.make_async_copy(src, dst, table_sem.at[spot])
        copy.start()
        table_copies.append(copy)

    for copy in table_copies:
        copy.wait()
    low_digit = lax.broadcasted_iota(jnp.int32, (A, 128), 0)
    high_digit = lax.broadcasted_iota(jnp.int32, (A, 128), 1)
    frequency = low_digit + A * high_digit
    signed = jnp.where(frequency < total // 2, frequency, frequency - total).astype(f32)
    omega = signed * (8.0 / total)
    for m in range(ml):
        phase = (
            beta[0, m, kind[0]] * omega
            + beta[1, m, kind[0]] * (omega * omega) / 2.0
            + beta[2, m, kind[0]] * (omega * omega * omega) / 6.0
        )
        phase_tab[0, m * A : (m + 1) * A, :] = jnp.cos(phase)
        phase_tab[1, m * A : (m + 1) * A, :] = jnp.sin(phase)
    def disperse(stacked, direction, modes):
        spun = left_dot(left_f, stacked)
        tw_r, tw_i = twist[0], twist[1]
        blocks = []
        for m in range(len(modes)):
            re = spun[:A, m * 128 : (m + 1) * 128]
            im = spun[A:, m * 128 : (m + 1) * 128]
            blocks.append(jnp.concatenate([re * tw_r - im * tw_i, re * tw_i + im * tw_r], axis=1))
        spectrum = right_dot(jnp.concatenate(blocks, axis=0), right_f)
        re, im = spectrum[:, :128], spectrum[:, 128:]
        cosine, sine = (
            jnp.concatenate([phase_tab[part, m * A : (m + 1) * A, :] for m in modes], axis=0) for part in range(2)
        )
        sine = sine * direction
        turned = jnp.concatenate([re * cosine - im * sine, re * sine + im * cosine], axis=1)
        back = right_dot(turned, right_i)
        real_rows, imag_rows = [], []
        for m in range(len(modes)):
            re = back[m * A : (m + 1) * A, :128]
            im = back[m * A : (m + 1) * A, 128:]
            real_rows.append(re * tw_r + im * tw_i)
            imag_rows.append(im * tw_r - re * tw_i)
        joined = jnp.concatenate(
            [jnp.concatenate(real_rows, axis=1), jnp.concatenate(imag_rows, axis=1)], axis=0
        )
        return left_dot(left_i, joined)

    def send_gradient(b, h, m, peer):
        rows = pl.ds(h * Hk, Hk)
        go(
            grads.at[b, peer * ml + m, :, rows], rows_back.at[b, m, me_m, :, rows],
            gb_s.at[b, h, m, peer], gb_r.at[b, h, m, me_m], "mode", peer,
        )

    def line_up(b):
        @pl.loop(0, M)
        def _(p):
            owner, local = p // ml, lax.rem(p, ml)
            for ri in range(2):
                wanted[p, ri] = jnp.concatenate(
                    [t2[b][j, owner, ri, pl.ds(local, As, stride=ml), :] for j in range(Dt)], axis=0
                )

    def kerr(b, h):
        field = kb[b * parts + h]
        tiles = Hk // 8
        depth = J * 8

        for j in range(0, J, 2):
            made = []
            for s in range(2):
                first, second = pairs[0, j + s], pairs[1, j + s]
                ar, ai = field[first, 0], field[first, 1]
                br, bi = field[second, 0], field[second, 1]
                made.append((ar * br - ai * bi, ar * bi + ai * br))
            for q in range(tiles):
                for ri in range(2):
                    high, low = halves(
                        jnp.concatenate([made[s][ri][q * 8 : q * 8 + 8] for s in range(2)], axis=0)
                    )
                    cols = pl.ds((2 * q + ri) * 128, 128)
                    pair_cols[j * 8 : j * 8 + 16, cols] = high
                    pair_cols[depth + j * 8 : depth + j * 8 + 16, cols] = low
                    pair_cols[2 * depth + j * 8 : 2 * depth + j * 8 + 16, cols] = high
        for q in range(tiles):
            cols = pl.ds(q * 256, 256)
            coup[:, cols] = mm(w1[...], pair_cols[:, cols])

        @pl.loop(0, M // 2)
        def _(pp):
            for q in range(tiles):
                rows, here = pl.ds(h * Hk + q * 8, 8), pl.ds(q * 8, 8)
                pushed = []
                for s in range(2):
                    p = pp * 2 + s
                    kr = ki = jnp.zeros((8, 128), f32)
                    for n in range(M):
                        at = pl.ds(pl.multiple_of((p * M + n) * 8, 8), 8)
                        cr, ci = coup[at, q * 256 : q * 256 + 128], coup[at, q * 256 + 128 : q * 256 + 256]
                        ur, ui = field[n, 0, here], field[n, 1, here]
                        kr = kr + (cr * ur + ci * ui)
                        ki = ki + (ci * ur - cr * ui)
                    cr = 2.0 * (field[p, 0, here] - kerr_scale * ki - wanted[p, 0, rows])
                    ci = 2.0 * (field[p, 1, here] + kerr_scale * kr - wanted[p, 1, rows])
                    cots[p, 0, rows] = cr
                    cots[p, 1, rows] = ci
                    pushed.append((kerr_scale * ci, -kerr_scale * cr))
                    push[p, 0, rows] = pushed[s][0]
                    push[p, 1, rows] = pushed[s][1]
                for ri in range(2):
                    high, low = halves(jnp.concatenate([pushed[s][ri] for s in range(2)], axis=0))
                    cols = pl.ds((2 * q + ri) * 128, 128)
                    for part, value in enumerate((high, low, high)):
                        push_cols[pl.ds(pl.multiple_of(part * (M * 8) + pp * 16, 16), 16), cols] = value

        for q in range(tiles):
            cols = pl.ds(q * 256, 256)
            turn[:, cols] = mm(w2[...], push_cols[:, cols])

        @pl.loop(0, M)
        def _(n):
            for q in range(tiles):
                rows, here = pl.ds(h * Hk + q * 8, 8), pl.ds(q * 8, 8)
                gr, gi = cots[n, 0, rows], cots[n, 1, rows]
                for p in range(M):
                    at = pl.ds(pl.multiple_of((p * M + n) * 8, 8), 8)
                    cr, ci = coup[at, q * 256 : q * 256 + 128], coup[at, q * 256 + 128 : q * 256 + 256]
                    er, ei = push[p, 0, rows], push[p, 1, rows]
                    gr = gr + (er * cr + ei * ci)
                    gi = gi + (er * ci - ei * cr)
                cots[n, 0, rows] = gr
                cots[n, 1, rows] = gi

        @pl.loop(0, J // 2)
        def _(jj):
            for q in range(tiles):
                rows, here = pl.ds(h * Hk + q * 8, 8), pl.ds(q * 8, 8)
                moved = []
                for s in range(2):
                    j = jj * 2 + s
                    gr = gi = jnp.zeros((8, 128), f32)
                    for n in range(M):
                        at = pl.ds(pl.multiple_of((n * J + j) * 8, 8), 8)
                        tr, ti = turn[at, q * 256 : q * 256 + 128], turn[at, q * 256 + 128 : q * 256 + 256]
                        ur, ui = field[n, 0, here], field[n, 1, here]
                        gr = gr + (tr * ur - ti * ui)
                        gi = gi + (tr * ui + ti * ur)
                    for side in range(2):
                        other = pairs[1 - side, j]
                        vr, vi = field[other, 0, here], field[other, 1, here]
                        moved.append((side, (vr * gr + vi * gi, vr * gi - vi * gr)))
                for side in range(2):
                    for ri in range(2):
                        high, low = halves(
                            jnp.concatenate([value[ri] for which, value in moved if which == side], axis=0)
                        )
                        cols = pl.ds((2 * q + ri) * 128, 128)
                        at = side * depth + jj * 16
                        move_cols[pl.ds(pl.multiple_of(at, 16), 16), cols] = high
                        move_cols[pl.ds(pl.multiple_of(2 * depth + at, 16), 16), cols] = low

        for q in range(tiles):
            rows = pl.ds(h * Hk + q * 8, 8)
            back = mm(spread[...], move_cols[:, q * 256 : q * 256 + 256])
            for n in range(M):
                for ri in range(2):
                    grads[b, n, ri, rows] = (
                        cots[n, ri, rows] + back[n * 8 : n * 8 + 8, ri * 128 : ri * 128 + 128]
                    )

    for b in range(Bl):
        owns[("in", b)].wait()
        for peer in tm_peers:
            remote(x_near.at[:, b], rows_in.at[b, peer], in_s.at[b, peer], in_r.at[b, peer], "tm", peer).wait_recv()
        stacked = jnp.concatenate(
            [
                jnp.concatenate(
                    [rows_in[b, j, ri, pl.ds(m, Al, stride=ml), :] for ri in range(2) for j in range(Dt)], axis=0
                )
                for m in range(ml)
            ],
            axis=1,
        )
        result = disperse(stacked, 1.0, range(ml))
        for i in range(Dm):
            for m in range(ml):
                for ri in range(2):
                    for j in range(Dt):
                        row = ri * A + j * Al + i * As
                        h, at = j * As // Hk, j * As % Hk
                        send_z[i, b, h, m, ri, at : at + As, :] = result[row : row + As, m * 128 : (m + 1) * 128]
        for h in range(parts):
            for peer in mode_peers:
                go(
                    send_z.at[peer, b, h], kb[b * parts + h].at[pl.ds(me_m * ml, ml)],
                    kb_s.at[b, h, peer], kb_r.at[b, h, me_m], "mode", peer,
                )
            own(("kb", b, h), send_z.at[me_m, b, h], kb[b * parts + h].at[pl.ds(me_m * ml, ml)])
        if b == 0:
            target_second_leg(0)

    owns["mg"].wait()
    for peer in mode_peers:
        remote(margin, mg.at[peer], mg_ss.at[peer], mg_r.at[peer], "mode", peer).wait_recv()
    make_weights(sizes, pairs, mg, w1, w2, spread)
    for b in range(1, Bl):
        target_second_leg(b)

    for b in range(Bl):
        owns[("t2", b)].wait()
        for peer in tm_peers:
            remote(t1[b].at[:, :, 0], t2[b].at[peer], t2_s.at[b, peer], t2_r.at[b, peer], "tm", peer).wait_recv()
        line_up(b)
        for h in range(parts):
            owns[("kb", b, h)].wait()
            for peer in mode_peers:
                remote(
                    send_z.at[0, b, h], kb[b * parts + h].at[pl.ds(peer * ml, ml)],
                    kb_s.at[b, h, peer], kb_r.at[b, h, peer], "mode", peer,
                ).wait_recv()
            kerr(b, h)
            if b + 1 < Bl:
                for m in range(ml):
                    for peer in mode_peers:
                        send_gradient(b, h, m, peer)
        if b + 1 == Bl:
            for peer in mode_peers:
                for m in range(ml):
                    for h in range(parts):
                        send_gradient(b, h, m, peer)
        for m in range(ml):
            own(("gb", b, m), grads.at[b, me_m * ml + m], rows_back.at[b, m, me_m])

    for b in range(Bl):
        for m in range(ml):
            owns[("gb", b, m)].wait()
            for peer in mode_peers:
                for h in range(parts):
                    rows = pl.ds(h * Hk, Hk)
                    remote(
                        grads.at[b, m, :, rows], rows_back.at[b, m, peer, :, rows],
                        gb_s.at[b, h, m, peer], gb_r.at[b, h, m, peer], "mode", peer,
                    ).wait_recv()
            stacked = jnp.concatenate(
                [
                    rows_back[b, m, i, ri, j * As : (j + 1) * As, :]
                    for ri in range(2)
                    for j in range(Dt)
                    for i in range(Dm)
                ],
                axis=0,
            )
            result = disperse(stacked, -1.0, [m])
            for j in range(Dt):
                for ri in range(2):
                    row = ri * A + j * Al
                    send_out[j, b, m, ri] = result[row : row + Al, :]
            for peer in tm_peers:
                go(
                    send_out.at[peer, b, m], out.at[:, me_t * Bl + b, m],
                    out_s.at[b, m, peer], out_r.at[b, m, me_t], "tm", peer,
                )
            own(("out", b, m), send_out.at[me_t, b, m], out.at[:, me_t * Bl + b, m])
    for b in range(Bl):
        for m in range(ml):
            owns[("out", b, m)].wait()
            for peer in tm_peers:
                remote(
                    send_out.at[0, b, m], out.at[:, peer * Bl + b, m],
                    out_s.at[b, m, peer], out_r.at[b, m, peer], "tm", peer,
                ).wait_recv()
    for copy in sends:
        copy.wait_send()


def finish(gathered, out, woven, sem):
    _, B, ml, Al, _ = gathered.shape
    copies = []
    for b in range(B):
        for ri in range(2):
            for m in range(ml):
                woven[ri, b, pl.ds(m, Al, stride=ml), :] = gathered[ri, b, m]
        copy = pltpu.make_async_copy(woven.at[:, b], out.at[:, b], sem.at[b])
        copy.start()
        copies.append(copy)
    for copy in copies:
        copy.wait()


def on_device(Dm, Dt, input_field, target_field, margin, pair_index, mode_beta, segment_kind):
    _, B, ml, Tl = input_field.shape
    M, J = margin.shape[1], margin.shape[2]
    total = Tl * Dt
    A = total // 128
    Al = Tl // 128
    Bl = B // Dt
    As = Al // Dm
    Ak = As * Dt
    parts = 2 if Ak % 16 == 0 else 1
    Hk = Ak // parts
    def by_rows(values):
        return values.reshape(2, B, ml, Al, 128).transpose(0, 1, 3, 2, 4).reshape(2, B, Al * ml, 128)

    x = by_rows(input_field)
    target = by_rows(target_field).reshape(2, Dt, Bl, Al * ml, 128)
    if (As * ml) % 8:
        target = target.reshape(2, Dt, Bl, Dm, As * ml, 128).transpose(3, 0, 1, 2, 4, 5)
    tables = make_tables(A, total)
    sizes = (Dt, Dm, B, Bl, ml, M, A, Al, As, Ak, J, total)
    vm = lambda *shape: pltpu.VMEM(shape, f32)
    vb = lambda *shape: pltpu.VMEM(shape, bf16)
    dma = lambda *shape: pltpu.SemaphoreType.DMA(shape)
    anyspace = pl.BlockSpec(memory_space=pl.ANY)
    vmem = pl.BlockSpec(memory_space=pltpu.VMEM)
    gathered = pl.pallas_call(
        functools.partial(kernel, sizes),
        out_shape=pltpu.VMEM((2, B, ml, Al, 128), f32),
        in_specs=[anyspace] * 11,
        out_specs=vmem,
        scratch_shapes=[
            vm(*x.shape),
            vm(*target.shape),
            pltpu.SMEM(segment_kind.shape, jnp.int32),
            pltpu.SMEM(pair_index.shape[::-1], jnp.int32),
            vm(ml, M, J),
        ]
        + [pltpu.VMEM(t.shape, bf16) for t in tables[:4]]
        + [
            vm(2, A, 128),
            pltpu.SMEM((3, ml, mode_beta.shape[0]), f32),
            vm(2, ml * A, 128),
            vm(Bl, Dt, 2, Al * ml, 128),
            vm(Dm, Bl, parts, ml, 2, Hk, 128),
            [vm(M, 2, Hk, 128) for _ in range(Bl * parts)],
            [vm(Dm, 2, Dt, As * ml, 128) for _ in range(Bl)],
            [vm(Dt, Dm, 2, As * ml, 128) for _ in range(Bl)],
            vm(Dm, ml, M, J),
            vb(M * M * 8, 3 * J * 8),
            vb(M * J * 8, 3 * M * 8),
            vb(M * 8, 4 * J * 8),
            vb(3 * J * 8, Hk * 32),
            vm(M * M * 8, Hk * 32),
            vm(M, 2, Ak, 128),
            vm(M, 2, Ak, 128),
            vm(M, 2, Ak, 128),
            vb(3 * M * 8, Hk * 32),
            vm(M * J * 8, Hk * 32),
            vb(4 * J * 8, Hk * 32),
            vm(Bl, M, 2, Ak, 128),
            vm(Bl, ml, Dm, 2, Ak, 128),
            vm(Dt, Bl, ml, 2, Al, 128),
            dma(5),
            dma(6),
            dma((3 + parts + 2 * ml) * Bl + 1),
            dma(Bl, Dt), dma(Bl, Dt),
            dma(Dm), dma(Dm),
            dma(Bl, Dm), dma(Bl, Dm),
            dma(Bl, Dt), dma(Bl, Dt),
            dma(Bl, parts, Dm), dma(Bl, parts, Dm),
            dma(Bl, parts, ml, Dm), dma(Bl, parts, ml, Dm),
            dma(Bl, ml, Dt), dma(Bl, ml, Dt),
        ],
        compiler_params=pltpu.CompilerParams(collective_id=0, has_side_effects=True, vmem_limit_bytes=62 * 1024 * 1024),
    )(segment_kind, pair_index.T, x, target, margin, mode_beta.transpose(2, 1, 0), *[jnp.asarray(t) for t in tables])
    out = pl.pallas_call(
        finish,
        out_shape=jax.ShapeDtypeStruct((2, B, Al * ml, 128), f32),
        in_specs=[vmem],
        out_specs=anyspace,
        scratch_shapes=[vm(2, B, Al * ml, 128), dma(B)],
    )(pltpu.with_memory_space_constraint(gathered, pltpu.VMEM))
    return out.reshape(2, B, Al, ml, 128).transpose(0, 1, 3, 2, 4).reshape(2, B, ml, Tl)


def solution(mesh):
    return jax.shard_map(
        functools.partial(on_device, mesh.shape["mode"], mesh.shape["tm"]),
        mesh=mesh,
        in_specs=(
            P(None, "dp", "mode", "tm"),
            P(None, "dp", "mode", "tm"),
            P("mode", None, None),
            P(),
            P(None, "mode", None),
            P(),
        ),
        out_specs=P(None, "dp", "mode", "tm"),
        check_vma=False,
    )
```

```python
import functools
import math

import jax
import jax.numpy as jnp
import numpy as np
from jax import lax
from jax.experimental import pallas as pl
from jax.experimental.pallas import tpu as pltpu
from jax.sharding import PartitionSpec as P

kerr_scale = 0.1
MESH = pl.DeviceIdType.MESH
f32 = jnp.float32
bf16 = jnp.bfloat16


def split_table(table):
    high = table.astype(np.float32).astype(bf16)
    low = (table - high.astype(np.float64)).astype(np.float32).astype(bf16)
    return np.stack([np.asarray(high), np.asarray(low)])


def real_form(size):
    turns = np.outer(np.arange(size), np.arange(size)) % size
    angle = turns * (2.0 * math.pi / size)
    cosine, sine = np.cos(angle), np.sin(angle)
    return np.block([[cosine, sine], [-sine, cosine]])


def make_tables(outer, total):
    left, right = real_form(outer), real_form(128)
    turns = np.outer(np.arange(outer), np.arange(128)) % total
    angle = turns * (2.0 * math.pi / total)
    twist = np.stack([np.cos(angle), -np.sin(angle)]).astype(np.float32)
    return (
        split_table(left),
        split_table(left.T / total),
        split_table(right.T),
        split_table(right),
        twist,
    )


def halves(value):
    high = value.astype(bf16)
    return high, (value - high.astype(f32)).astype(bf16)


def mm(a, b):
    return jnp.dot(a, b, preferred_element_type=f32)


def left_dot(table, value):
    high, low = halves(value)
    return mm(table[0], high) + (mm(table[0], low) + mm(table[1], high))


def right_dot(value, table):
    high, low = halves(value)
    return mm(high, table[0]) + (mm(low, table[0]) + mm(high, table[1]))


def farthest_first(me, count):
    low, high = jnp.int32(0), jnp.int32(count - 1)
    peers = []
    for _ in range(count - 1):
        up = (high - me >= me - low).astype(jnp.int32)
        peers.append(up * high + (1 - up) * low)
        high, low = high - up, low + 1 - up
    return peers


def digits(shape, axis):
    return lax.broadcasted_iota(jnp.int32, shape, axis)


def one_hot(condition):
    return jnp.where(condition, 1.0, 0.0).astype(bf16)


def make_weights(sizes, pairs, mg, w1, w2, spread):
    Dt, Dm, B, Bl, ml, M, A, Al, As, Ak, J, total = sizes
    depth = J * 8
    group = max(1, 64 // M)
    step = group * M

    rows, cols = digits((step * 8, step), 0), digits((step * 8, step), 1)
    taller = one_hot(rows // 8 == cols)
    rows, cols = digits((2 * J, 3 * depth), 0), digits((2 * J, 3 * depth), 1)
    wider = one_hot((rows == cols % depth // 8 + jnp.where(cols < 2 * depth, 0, J)))
    kept = digits((step * 8, 3 * depth), 0) % 8 == digits((step * 8, 3 * depth), 1) % 8

    def block(p):
        return mg[p // ml, p % ml]

    columns = []
    for g in range(M // group):
        values = jnp.concatenate([block(g * group + i) for i in range(group)], axis=0)
        high, low = halves(values)
        both = jnp.concatenate([high.astype(f32), low.astype(f32)], axis=1).astype(bf16)
        tall = mm(taller, both).astype(bf16)
        wide = mm(tall, wider)
        w1[g * step * 8 : (g + 1) * step * 8, :] = jnp.where(kept, wide, 0.0).astype(bf16)
        columns.append((high, low))

    rows, cols = digits((depth, J), 0), digits((depth, J), 1)
    lifter = one_hot(rows // 8 == cols)

    def turned(values):
        return lax.dot_general(lifter, values, (((1,), (1,)), ((), ())), preferred_element_type=f32).astype(bf16)

    lifted = [[turned(part) for part in pair] for pair in columns]
    width = M * 8
    kept = digits((depth, 3 * width), 0) % 8 == digits((depth, 3 * width), 1) % 8
    rows, cols = digits((step, 3 * width), 0), digits((step, 3 * width), 1)

    def fill(n):
        total = jnp.zeros((depth, 3 * width), f32)
        for g, parts in enumerate(lifted):
            for which, part in enumerate(parts):
                inside = (cols >= 2 * width) if which else (cols < 2 * width)
                match = (rows // M + g * group == cols % width // 8) & (rows % M == n) & inside
                total = total + mm(part, one_hot(match))
        w2[pl.ds(pl.multiple_of(n * depth, depth), depth), :] = jnp.where(kept, total, 0.0).astype(bf16)

    if M <= 8:
        for n in range(M):
            fill(n)
    else:
        pl.loop(0, M)(fill)

    which = digits((8, 2 * depth), 1) // 8
    chosen = jnp.zeros((8, 2 * depth), jnp.int32)
    for side in range(2):
        for j in range(J):
            chosen = jnp.where(which == side * J + j, pairs[side, j], chosen)
    shape = (width, 2 * depth)
    match = (digits(shape, 0) // 8 == jnp.concatenate([chosen] * M, axis=0)) & (
        digits(shape, 0) % 8 == digits(shape, 1) % 8
    )
    spread[:, : 2 * depth] = one_hot(match)
    spread[:, 2 * depth :] = one_hot(match)


def kernel(
    sizes, kind_hbm, pairs_hbm, x, target, margin_hbm, beta_hbm,
    left_f_hbm, left_i_hbm, right_f_hbm, right_i_hbm, twist_hbm, out,
    x_near, target_near, kind, pairs, margin, left_f, left_i, right_f, right_i, twist, beta, phase_tab,
    rows_in, send_z, kb, t1, t2, mg, w1, w2, spread, pair_cols, coup, wanted, cots, push, push_cols, turn, direct, move_cols,
    grads, rows_back, send_out,
    near_sem, table_sem, sent, in_r, mg_r, t1_r, t2_r, kb_r, gb_r, out_r,
):
    Dt, Dm, B, Bl, ml, M, A, Al, As, Ak, J, total = sizes
    parts = 2 if Ak % 16 == 0 else 1
    Hk = Ak // parts
    me_t = lax.axis_index("tm")
    me_m = lax.axis_index("mode")
    tm_peers = farthest_first(me_t, Dt)
    mode_peers = farthest_first(me_m, Dm)

    def remote(src, dst, send, recv, axis, peer):
        return pltpu.make_async_remote_copy(
            src_ref=src, dst_ref=dst, send_sem=send, recv_sem=recv, device_id={axis: peer}, device_id_type=MESH
        )

    barrier = pltpu.get_barrier_semaphore()
    for peer in mode_peers:
        pl.semaphore_signal(barrier, inc=1, device_id={"mode": peer}, device_id_type=MESH)
    for peer in tm_peers:
        pl.semaphore_signal(barrier, inc=1, device_id={"tm": peer}, device_id_type=MESH)
    staged = []
    for spot, (src, dst) in enumerate(
        ((margin_hbm, margin), (target, target_near), (x, x_near), (kind_hbm, kind), (pairs_hbm, pairs))
    ):
        staged.append(pltpu.make_async_copy(src, dst, near_sem.at[spot]))
        staged[-1].start()
    pl.semaphore_wait(barrier, Dt + Dm - 2)

    def go(src, dst, leg, recv, axis, peer):
        remote(src, dst, sent.at[leg], recv, axis, peer).start()

    def own(src, dst, recv):
        pltpu.make_async_copy(src, dst, recv).start()

    def arrived(whole, recv):
        pltpu.make_async_copy(whole, whole, recv).wait()

    def target_part(i, b):
        if (As * ml) % 8 == 0:
            return target_near.at[:, :, b, pl.ds(pl.multiple_of(i * (As * ml), 8), As * ml), :]
        return target_near.at[i, :, :, b]

    def target_first_leg(b):
        for peer in mode_peers:
            go(target_part(peer, b), t1.at[b, me_m], 2, t1_r.at[b], "mode", peer)
        own(target_part(me_m, b), t1.at[b, me_m], t1_r.at[b])

    def target_second_leg(b):
        arrived(t1.at[b], t1_r.at[b])
        for peer in tm_peers:
            go(t1.at[b, :, :, peer], t2.at[b, me_t], 3, t2_r.at[b], "tm", peer)
        own(t1.at[b, :, :, me_t], t2.at[b, me_t], t2_r.at[b])

    staged[0].wait()
    for peer in mode_peers:
        go(margin, mg.at[me_m], 1, mg_r, "mode", peer)
    own(margin, mg.at[me_m], mg_r)
    staged[1].wait()
    target_first_leg(0)
    staged[2].wait()
    for b in range(Bl):
        for peer in tm_peers:
            go(x_near.at[:, peer * Bl + b], rows_in.at[b, me_t], 0, in_r.at[b], "tm", peer)
        own(x_near.at[:, me_t * Bl + b], rows_in.at[b, me_t], in_r.at[b])
    for b in range(1, Bl):
        target_first_leg(b)
    for copy in staged[3:]:
        copy.wait()
    table_copies = []
    for spot, (src, dst) in enumerate(
        ((left_f_hbm, left_f), (left_i_hbm, left_i), (right_f_hbm, right_f), (right_i_hbm, right_i), (twist_hbm, twist), (beta_hbm, beta))
    ):
        copy = pltpu.make_async_copy(src, dst, table_sem.at[spot])
        copy.start()
        table_copies.append(copy)

    for copy in table_copies:
        copy.wait()
    low_digit = lax.broadcasted_iota(jnp.int32, (A, 128), 0)
    high_digit = lax.broadcasted_iota(jnp.int32, (A, 128), 1)
    frequency = low_digit + A * high_digit
    signed = jnp.where(frequency < total // 2, frequency, frequency - total).astype(f32)
    omega = signed * (8.0 / total)
    for m in range(ml):
        phase = (
            beta[0, m, kind[0]] * omega
            + beta[1, m, kind[0]] * (omega * omega) / 2.0
            + beta[2, m, kind[0]] * (omega * omega * omega) / 6.0
        )
        phase_tab[0, m * A : (m + 1) * A, :] = jnp.cos(phase)
        phase_tab[1, m * A : (m + 1) * A, :] = jnp.sin(phase)
    def disperse(stacked, direction, modes):
        spun = left_dot(left_f, stacked)
        tw_r, tw_i = twist[0], twist[1]
        blocks = []
        for m in range(len(modes)):
            re = spun[:A, m * 128 : (m + 1) * 128]
            im = spun[A:, m * 128 : (m + 1) * 128]
            blocks.append(jnp.concatenate([re * tw_r - im * tw_i, re * tw_i + im * tw_r], axis=1))
        spectrum = right_dot(jnp.concatenate(blocks, axis=0), right_f)
        re, im = spectrum[:, :128], spectrum[:, 128:]
        cosine, sine = (
            jnp.concatenate([phase_tab[part, m * A : (m + 1) * A, :] for m in modes], axis=0) for part in range(2)
        )
        sine = sine * direction
        turned = jnp.concatenate([re * cosine - im * sine, re * sine + im * cosine], axis=1)
        back = right_dot(turned, right_i)
        real_rows, imag_rows = [], []
        for m in range(len(modes)):
            re = back[m * A : (m + 1) * A, :128]
            im = back[m * A : (m + 1) * A, 128:]
            real_rows.append(re * tw_r + im * tw_i)
            imag_rows.append(im * tw_r - re * tw_i)
        joined = jnp.concatenate(
            [jnp.concatenate(real_rows, axis=1), jnp.concatenate(imag_rows, axis=1)], axis=0
        )
        return left_dot(left_i, joined)

    def send_gradient(b, h, m, peer):
        rows = pl.ds(h * Hk, Hk)
        go(
            grads.at[b, peer * ml + m, :, rows], rows_back.at[b, m, me_m, :, rows],
            5, gb_r.at[b, m], "mode", peer,
        )

    def line_up(b):
        @pl.loop(0, M)
        def _(p):
            owner, local = p // ml, lax.rem(p, ml)
            for ri in range(2):
                wanted[p, ri] = jnp.concatenate(
                    [t2[b, j, owner, ri, pl.ds(local, As, stride=ml), :] for j in range(Dt)], axis=0
                )

    def each(count, body):
        if M <= 8:
            for i in range(count):
                body(i)
        else:
            pl.loop(0, count)(body)

    def span(start, size):
        return pl.ds(start if isinstance(start, int) else pl.multiple_of(start, size), size)

    def kerr(b, h):
        field = kb[b * parts + h]
        tiles = Hk // 8
        depth = J * 8

        def block(ref, row, q):
            return [ref[span(row * 8, 8), (2 * q + ri) * 128 : (2 * q + ri + 1) * 128] for ri in range(2)]

        def put(ref, start, q, ri, value):
            ref[span(start, 16), (2 * q + ri) * 128 : (2 * q + ri + 1) * 128] = value

        def multiply_pairs(q):
            here = pl.ds(q * 8, 8)
            for j in range(0, J, 2):
                made = []
                for s in range(2):
                    first, second = pairs[0, j + s], pairs[1, j + s]
                    ar, ai = field[first, 0, here], field[first, 1, here]
                    br, bi = field[second, 0, here], field[second, 1, here]
                    made.append((ar * br - ai * bi, ar * bi + ai * br))
                for ri in range(2):
                    high, low = halves(jnp.concatenate([value[ri] for value in made], axis=0))
                    for part, value in enumerate((high, low, high)):
                        put(pair_cols, part * depth + j * 8, q, ri, value)

        def couple(q):
            cols = pl.ds(q * 256, 256)
            coup[:, cols] = mm(w1[...], pair_cols[:, cols])

        def compare(q):
            rows, here = pl.ds(h * Hk + q * 8, 8), pl.ds(q * 8, 8)

            def body(pp):
                pushed = []
                for s in range(2):
                    p = pp * 2 + s
                    kr = ki = jnp.zeros((8, 128), f32)
                    for n in range(M):
                        cr, ci = block(coup, p * M + n, q)
                        ur, ui = field[n, 0, here], field[n, 1, here]
                        kr = kr + (cr * ur + ci * ui)
                        ki = ki + (ci * ur - cr * ui)
                    cr = 2.0 * (field[p, 0, here] - kerr_scale * ki - wanted[p, 0, rows])
                    ci = 2.0 * (field[p, 1, here] + kerr_scale * kr - wanted[p, 1, rows])
                    cots[p, 0, rows] = cr
                    cots[p, 1, rows] = ci
                    pushed.append((kerr_scale * ci, -kerr_scale * cr))
                    push[p, 0, rows] = pushed[s][0]
                    push[p, 1, rows] = pushed[s][1]
                for ri in range(2):
                    high, low = halves(jnp.concatenate([value[ri] for value in pushed], axis=0))
                    for part, value in enumerate((high, low, high)):
                        put(push_cols, part * (M * 8) + pp * 16, q, ri, value)

            each(M // 2, body)

        def turn_back(q):
            cols = pl.ds(q * 256, 256)
            turn[:, cols] = mm(w2[...], push_cols[:, cols])

        def through_conjugate(q):
            rows = pl.ds(h * Hk + q * 8, 8)

            def body(n):
                gr, gi = cots[n, 0, rows], cots[n, 1, rows]
                for p in range(M):
                    cr, ci = block(coup, p * M + n, q)
                    er, ei = push[p, 0, rows], push[p, 1, rows]
                    gr = gr + (er * cr + ei * ci)
                    gi = gi + (er * ci - ei * cr)
                direct[n, 0, rows] = gr
                direct[n, 1, rows] = gi

            each(M, body)

        def through_pairs(q):
            here = pl.ds(q * 8, 8)

            def body(jj):
                moved = [[], []]
                for s in range(2):
                    j = jj * 2 + s
                    gr = gi = jnp.zeros((8, 128), f32)
                    for n in range(M):
                        tr, ti = block(turn, n * J + j, q)
                        ur, ui = field[n, 0, here], field[n, 1, here]
                        gr = gr + (tr * ur - ti * ui)
                        gi = gi + (tr * ui + ti * ur)
                    for side in range(2):
                        other = pairs[1 - side, j]
                        vr, vi = field[other, 0, here], field[other, 1, here]
                        moved[side].append((vr * gr + vi * gi, vr * gi - vi * gr))
                for side in range(2):
                    for ri in range(2):
                        high, low = halves(jnp.concatenate([value[ri] for value in moved[side]], axis=0))
                        put(move_cols, side * depth + jj * 16, q, ri, high)
                        put(move_cols, (2 + side) * depth + jj * 16, q, ri, low)

            each(J // 2, body)

        def gather(q):
            rows = pl.ds(h * Hk + q * 8, 8)
            back = mm(spread[...], move_cols[:, q * 256 : q * 256 + 256])
            for n in range(M):
                for ri in range(2):
                    grads[b, n, ri, rows] = (
                        direct[n, ri, rows] + back[n * 8 : n * 8 + 8, ri * 128 : ri * 128 + 128]
                    )

        for q in range(tiles):
            multiply_pairs(q)
        for q in range(tiles):
            couple(q)
        for q in range(tiles):
            compare(q)
            turn_back(q)
        for q in range(tiles):
            through_conjugate(q)
            through_pairs(q)
            gather(q)

    for b in range(Bl):
        arrived(rows_in.at[b], in_r.at[b])
        stacked = jnp.concatenate(
            [
                jnp.concatenate(
                    [rows_in[b, j, ri, pl.ds(m, Al, stride=ml), :] for ri in range(2) for j in range(Dt)], axis=0
                )
                for m in range(ml)
            ],
            axis=1,
        )
        result = disperse(stacked, 1.0, range(ml))
        for i in range(Dm):
            for m in range(ml):
                for ri in range(2):
                    for j in range(Dt):
                        row = ri * A + j * Al + i * As
                        h, at = j * As // Hk, j * As % Hk
                        send_z[i, b, h, m, ri, at : at + As, :] = result[row : row + As, m * 128 : (m + 1) * 128]
        for h in range(parts):
            for peer in mode_peers:
                go(
                    send_z.at[peer, b, h], kb[b * parts + h].at[pl.ds(me_m * ml, ml)],
                    4, kb_r.at[b, h], "mode", peer,
                )
            own(send_z.at[me_m, b, h], kb[b * parts + h].at[pl.ds(me_m * ml, ml)], kb_r.at[b, h])
        if b == 0:
            target_second_leg(0)

    arrived(mg, mg_r)
    make_weights(sizes, pairs, mg, w1, w2, spread)
    for b in range(1, Bl):
        target_second_leg(b)

    for b in range(Bl):
        arrived(t2.at[b], t2_r.at[b])
        line_up(b)
        for h in range(parts):
            arrived(kb[b * parts + h], kb_r.at[b, h])
            kerr(b, h)
            if b + 1 < Bl:
                for m in range(ml):
                    for peer in mode_peers:
                        send_gradient(b, h, m, peer)
        if b + 1 == Bl:
            for peer in mode_peers:
                for m in range(ml):
                    for h in range(parts):
                        send_gradient(b, h, m, peer)
        for m in range(ml):
            own(grads.at[b, me_m * ml + m], rows_back.at[b, m, me_m], gb_r.at[b, m])

    for b in range(Bl):
        for m in range(ml):
            arrived(rows_back.at[b, m], gb_r.at[b, m])
            stacked = jnp.concatenate(
                [
                    rows_back[b, m, i, ri, j * As : (j + 1) * As, :]
                    for ri in range(2)
                    for j in range(Dt)
                    for i in range(Dm)
                ],
                axis=0,
            )
            result = disperse(stacked, -1.0, [m])
            for j in range(Dt):
                for ri in range(2):
                    row = ri * A + j * Al
                    send_out[j, b, m, ri] = result[row : row + Al, :]
            for peer in tm_peers:
                go(
                    send_out.at[peer, b, m], out.at[:, me_t * Bl + b, m],
                    6, out_r, "tm", peer,
                )
            own(send_out.at[me_t, b, m], out.at[:, me_t * Bl + b, m], out_r)
    arrived(out, out_r)
    others_t, others_m = pl.ds(0, Dt - 1), pl.ds(0, Dm - 1)
    for leg, whole in enumerate(
        (
            rows_in.at[:, others_t],
            mg.at[others_m],
            t1.at[:, others_m],
            t2.at[:, others_t],
            send_z.at[others_m],
            rows_back.at[:, :, others_m],
            send_out.at[others_t],
        )
    ):
        arrived(whole, sent.at[leg])


def finish(gathered, out, sem):
    _, B, ml, _, _ = gathered.shape
    for b in range(B):
        for m in range(ml):
            pltpu.make_async_copy(gathered.at[:, b, m], out.at[:, b, :, m], sem).start()
    pltpu.make_async_copy(gathered, gathered, sem).wait()


def on_device(Dm, Dt, input_field, target_field, margin, pair_index, mode_beta, segment_kind):
    _, B, ml, Tl = input_field.shape
    M, J = margin.shape[1], margin.shape[2]
    total = Tl * Dt
    A = total // 128
    Al = Tl // 128
    Bl = B // Dt
    As = Al // Dm
    Ak = As * Dt
    parts = 2 if Ak % 16 == 0 else 1
    Hk = Ak // parts
    def by_rows(values):
        return values.reshape(2, B, ml, Al, 128).transpose(0, 1, 3, 2, 4).reshape(2, B, Al * ml, 128)

    x = by_rows(input_field)
    target = by_rows(target_field).reshape(2, Dt, Bl, Al * ml, 128)
    if (As * ml) % 8:
        target = target.reshape(2, Dt, Bl, Dm, As * ml, 128).transpose(3, 0, 1, 2, 4, 5)
    tables = make_tables(A, total)
    sizes = (Dt, Dm, B, Bl, ml, M, A, Al, As, Ak, J, total)
    vm = lambda *shape: pltpu.VMEM(shape, f32)
    vb = lambda *shape: pltpu.VMEM(shape, bf16)
    dma = lambda *shape: pltpu.SemaphoreType.DMA(shape)
    anyspace = pl.BlockSpec(memory_space=pl.ANY)
    gathered = pl.pallas_call(
        functools.partial(kernel, sizes),
        out_shape=pltpu.VMEM((2, B, ml, Al, 128), f32),
        in_specs=[anyspace] * 11,
        out_specs=anyspace,
        scratch_shapes=[
            vm(*x.shape),
            vm(*target.shape),
            pltpu.SMEM(segment_kind.shape, jnp.int32),
            pltpu.SMEM(pair_index.shape[::-1], jnp.int32),
            vm(ml, M, J),
        ]
        + [pltpu.VMEM(t.shape, bf16) for t in tables[:4]]
        + [
            vm(2, A, 128),
            pltpu.SMEM((3, ml, mode_beta.shape[0]), f32),
            vm(2, ml * A, 128),
            vm(Bl, Dt, 2, Al * ml, 128),
            vm(Dm, Bl, parts, ml, 2, Hk, 128),
            [vm(M, 2, Hk, 128) for _ in range(Bl * parts)],
            vm(Bl, Dm, 2, Dt, As * ml, 128),
            vm(Bl, Dt, Dm, 2, As * ml, 128),
            vm(Dm, ml, M, J),
            vb(M * M * 8, 3 * J * 8),
            vb(M * J * 8, 3 * M * 8),
            vb(M * 8, 4 * J * 8),
            vb(3 * J * 8, Hk * 32),
            vm(M * M * 8, Hk * 32),
            vm(M, 2, Ak, 128),
            vm(M, 2, Ak, 128),
            vm(M, 2, Ak, 128),
            vb(3 * M * 8, Hk * 32),
            vm(M * J * 8, Hk * 32),
            vm(M, 2, Ak, 128),
            vb(4 * J * 8, Hk * 32),
            vm(Bl, M, 2, Ak, 128),
            vm(Bl, ml, Dm, 2, Ak, 128),
            vm(Dt, Bl, ml, 2, Al, 128),
            dma(5),
            dma(6),
            dma(7),
            dma(Bl),
            dma(),
            dma(Bl),
            dma(Bl),
            dma(Bl, parts),
            dma(Bl, ml),
            dma(),
        ],
        compiler_params=pltpu.CompilerParams(collective_id=0, has_side_effects=True, vmem_limit_bytes=62 * 1024 * 1024),
    )(segment_kind, pair_index.T, x, target, margin, mode_beta.transpose(2, 1, 0), *[jnp.asarray(t) for t in tables])
    out = pl.pallas_call(
        finish,
        out_shape=jax.ShapeDtypeStruct((2, B, Al, ml, 128), f32),
        in_specs=[anyspace],
        out_specs=anyspace,
        scratch_shapes=[dma()],
    )(pltpu.with_memory_space_constraint(gathered, pltpu.VMEM))
    return out.transpose(0, 1, 3, 2, 4).reshape(2, B, ml, Tl)


def solution(mesh):
    return jax.shard_map(
        functools.partial(on_device, mesh.shape["mode"], mesh.shape["tm"]),
        mesh=mesh,
        in_specs=(
            P(None, "dp", "mode", "tm"),
            P(None, "dp", "mode", "tm"),
            P("mode", None, None),
            P(),
            P(None, "mode", None),
            P(),
        ),
        out_specs=P(None, "dp", "mode", "tm"),
        check_vma=False,
    )
```

```python
import functools
import math

import jax
import jax.numpy as jnp
import numpy as np
from jax import lax
from jax.experimental import pallas as pl
from jax.experimental.pallas import tpu as pltpu
from jax.sharding import PartitionSpec as P

kerr_scale = 0.1
MESH = pl.DeviceIdType.MESH
f32 = jnp.float32
bf16 = jnp.bfloat16


def split_table(table):
    high = table.astype(np.float32).astype(bf16)
    low = (table - high.astype(np.float64)).astype(np.float32).astype(bf16)
    return np.stack([np.asarray(high), np.asarray(low)])


def real_form(size):
    turns = np.outer(np.arange(size), np.arange(size)) % size
    angle = turns * (2.0 * math.pi / size)
    cosine, sine = np.cos(angle), np.sin(angle)
    return np.block([[cosine, sine], [-sine, cosine]])


def make_tables(outer, total):
    left, right = real_form(outer), real_form(128)
    turns = np.outer(np.arange(outer), np.arange(128)) % total
    angle = turns * (2.0 * math.pi / total)
    twist = np.stack([np.cos(angle), -np.sin(angle)]).astype(np.float32)
    return (
        split_table(left),
        split_table(left.T / total),
        split_table(right.T),
        split_table(right),
        twist,
    )


def halves(value):
    high = value.astype(bf16)
    return high, (value - high.astype(f32)).astype(bf16)


def mm(a, b):
    return jnp.dot(a, b, preferred_element_type=f32)


def left_dot(table, value):
    high, low = halves(value)
    width = value.shape[1]
    if width > 128:
        return mm(table[0], high) + (mm(table[0], low) + mm(table[1], high))
    both = mm(table[0], jnp.concatenate([high, low], axis=1))
    return both[:, :width] + (both[:, width:] + mm(table[1], high))


def right_dot(value, table):
    high, low = halves(value)
    rows = value.shape[0]
    both = mm(jnp.concatenate([high, low], axis=0), table[0])
    return both[:rows] + (both[rows:] + mm(high, table[1]))


def farthest_first(me, count):
    low, high = jnp.int32(0), jnp.int32(count - 1)
    peers = []
    for _ in range(count - 1):
        up = (high - me >= me - low).astype(jnp.int32)
        peers.append(up * high + (1 - up) * low)
        high, low = high - up, low + 1 - up
    return peers


def digits(shape, axis):
    return lax.broadcasted_iota(jnp.int32, shape, axis)


def one_hot(condition):
    return jnp.where(condition, 1.0, 0.0).astype(bf16)


def make_weights(sizes, pairs, mg, w1, w2, spread):
    Dt, Dm, B, Bl, ml, M, A, Al, As, Ak, J, total = sizes
    depth = J * 8
    group = max(1, 64 // M)
    step = group * M

    rows, cols = digits((step * 8, step), 0), digits((step * 8, step), 1)
    taller = one_hot(rows // 8 == cols)
    rows, cols = digits((2 * J, 3 * depth), 0), digits((2 * J, 3 * depth), 1)
    wider = one_hot((rows == cols % depth // 8 + jnp.where(cols < 2 * depth, 0, J)))
    kept = digits((step * 8, 3 * depth), 0) % 8 == digits((step * 8, 3 * depth), 1) % 8

    def block(p):
        return mg[p // ml, p % ml]

    columns = []
    for g in range(M // group):
        values = jnp.concatenate([block(g * group + i) for i in range(group)], axis=0)
        high, low = halves(values)
        both = jnp.concatenate([high.astype(f32), low.astype(f32)], axis=1).astype(bf16)
        tall = mm(taller, both).astype(bf16)
        wide = mm(tall, wider)
        w1[g * step * 8 : (g + 1) * step * 8, :] = jnp.where(kept, wide, 0.0).astype(bf16)
        columns.append((high, low))

    rows, cols = digits((depth, J), 0), digits((depth, J), 1)
    lifter = one_hot(rows // 8 == cols)

    def turned(values):
        return lax.dot_general(lifter, values, (((1,), (1,)), ((), ())), preferred_element_type=f32).astype(bf16)

    lifted = [[turned(part) for part in pair] for pair in columns]
    width = M * 8
    kept = digits((depth, 3 * width), 0) % 8 == digits((depth, 3 * width), 1) % 8
    rows, cols = digits((step, 3 * width), 0), digits((step, 3 * width), 1)

    def fill(n):
        total = jnp.zeros((depth, 3 * width), f32)
        for g, parts in enumerate(lifted):
            for which, part in enumerate(parts):
                inside = (cols >= 2 * width) if which else (cols < 2 * width)
                match = (rows // M + g * group == cols % width // 8) & (rows % M == n) & inside
                total = total + mm(part, one_hot(match))
        w2[pl.ds(pl.multiple_of(n * depth, depth), depth), :] = jnp.where(kept, total, 0.0).astype(bf16)

    if M <= 8:
        for n in range(M):
            fill(n)
    else:
        pl.loop(0, M)(fill)

    which = digits((8, 2 * depth), 1) // 8
    chosen = jnp.zeros((8, 2 * depth), jnp.int32)
    for side in range(2):
        for j in range(J):
            chosen = jnp.where(which == side * J + j, pairs[side, j], chosen)
    shape = (width, 2 * depth)
    match = (digits(shape, 0) // 8 == jnp.concatenate([chosen] * M, axis=0)) & (
        digits(shape, 0) % 8 == digits(shape, 1) % 8
    )
    spread[:, : 2 * depth] = one_hot(match)
    spread[:, 2 * depth :] = one_hot(match)


def kernel(
    sizes, kind_hbm, pairs_hbm, x, target, margin_hbm, beta_hbm,
    left_f_hbm, left_i_hbm, right_f_hbm, right_i_hbm, twist_hbm, out,
    x_near, target_near, kind, pairs, margin, left_f, left_i, right_f, right_i, twist, beta, phase_tab,
    rows_in, send_z, kb, t1, t2, mg, w1, w2, spread, pair_cols, coup, wanted, cots, push, push_cols, turn, direct, move_cols,
    grads, rows_back, send_out,
    near_sem, table_sem, sent, in_r, mg_r, t1_r, t2_r, kb_r, gb_r, out_r,
):
    Dt, Dm, B, Bl, ml, M, A, Al, As, Ak, J, total = sizes
    parts = 2 if Ak % 16 == 0 else 1
    Hk = Ak // parts
    me_t = lax.axis_index("tm")
    me_m = lax.axis_index("mode")
    tm_peers = farthest_first(me_t, Dt)
    mode_peers = farthest_first(me_m, Dm)

    def remote(src, dst, send, recv, axis, peer):
        return pltpu.make_async_remote_copy(
            src_ref=src, dst_ref=dst, send_sem=send, recv_sem=recv, device_id={axis: peer}, device_id_type=MESH
        )

    barrier = pltpu.get_barrier_semaphore()
    for peer in mode_peers:
        pl.semaphore_signal(barrier, inc=1, device_id={"mode": peer}, device_id_type=MESH)
    for peer in tm_peers:
        pl.semaphore_signal(barrier, inc=1, device_id={"tm": peer}, device_id_type=MESH)
    staged = []
    for spot, (src, dst) in enumerate(
        ((margin_hbm, margin), (target, target_near), (x, x_near), (kind_hbm, kind), (pairs_hbm, pairs))
    ):
        staged.append(pltpu.make_async_copy(src, dst, near_sem.at[spot]))
        staged[-1].start()
    pl.semaphore_wait(barrier, Dt + Dm - 2)

    def go(src, dst, leg, recv, axis, peer):
        remote(src, dst, sent.at[leg], recv, axis, peer).start()

    def own(src, dst, recv):
        pltpu.make_async_copy(src, dst, recv).start()

    def arrived(whole, recv):
        pltpu.make_async_copy(whole, whole, recv).wait()

    def target_part(i, b):
        if (As * ml) % 8 == 0:
            return target_near.at[:, :, b, pl.ds(pl.multiple_of(i * (As * ml), 8), As * ml), :]
        return target_near.at[i, :, :, b]

    def target_first_leg(b):
        for peer in mode_peers:
            go(target_part(peer, b), t1.at[b, me_m], 2, t1_r.at[b], "mode", peer)
        own(target_part(me_m, b), t1.at[b, me_m], t1_r.at[b])

    def target_second_leg(b):
        arrived(t1.at[b], t1_r.at[b])
        for peer in tm_peers:
            go(t1.at[b, :, :, peer], t2.at[b, me_t], 3, t2_r.at[b], "tm", peer)
        own(t1.at[b, :, :, me_t], t2.at[b, me_t], t2_r.at[b])

    staged[0].wait()
    for peer in mode_peers:
        go(margin, mg.at[me_m], 1, mg_r, "mode", peer)
    own(margin, mg.at[me_m], mg_r)
    staged[1].wait()
    target_first_leg(0)
    staged[2].wait()
    for b in range(Bl):
        for peer in tm_peers:
            go(x_near.at[:, peer * Bl + b], rows_in.at[b, me_t], 0, in_r.at[b], "tm", peer)
        own(x_near.at[:, me_t * Bl + b], rows_in.at[b, me_t], in_r.at[b])
    for b in range(1, Bl):
        target_first_leg(b)
    for copy in staged[3:]:
        copy.wait()
    table_copies = []
    for spot, (src, dst) in enumerate(
        ((left_f_hbm, left_f), (left_i_hbm, left_i), (right_f_hbm, right_f), (right_i_hbm, right_i), (twist_hbm, twist), (beta_hbm, beta))
    ):
        copy = pltpu.make_async_copy(src, dst, table_sem.at[spot])
        copy.start()
        table_copies.append(copy)

    for copy in table_copies:
        copy.wait()
    low_digit = lax.broadcasted_iota(jnp.int32, (A, 128), 0)
    high_digit = lax.broadcasted_iota(jnp.int32, (A, 128), 1)
    frequency = low_digit + A * high_digit
    signed = jnp.where(frequency < total // 2, frequency, frequency - total).astype(f32)
    omega = signed * (8.0 / total)
    for m in range(ml):
        phase = (
            beta[0, m, kind[0]] * omega
            + beta[1, m, kind[0]] * (omega * omega) / 2.0
            + beta[2, m, kind[0]] * (omega * omega * omega) / 6.0
        )
        phase_tab[0, m * A : (m + 1) * A, :] = jnp.cos(phase)
        phase_tab[1, m * A : (m + 1) * A, :] = jnp.sin(phase)
    def disperse(stacked, direction, modes):
        spun = left_dot(left_f, stacked)
        tw_r, tw_i = twist[0], twist[1]
        blocks = []
        for m in range(len(modes)):
            re = spun[:A, m * 128 : (m + 1) * 128]
            im = spun[A:, m * 128 : (m + 1) * 128]
            blocks.append(jnp.concatenate([re * tw_r - im * tw_i, re * tw_i + im * tw_r], axis=1))
        spectrum = right_dot(jnp.concatenate(blocks, axis=0), right_f)
        re, im = spectrum[:, :128], spectrum[:, 128:]
        cosine, sine = (
            jnp.concatenate([phase_tab[part, m * A : (m + 1) * A, :] for m in modes], axis=0) for part in range(2)
        )
        sine = sine * direction
        turned = jnp.concatenate([re * cosine - im * sine, re * sine + im * cosine], axis=1)
        back = right_dot(turned, right_i)
        real_rows, imag_rows = [], []
        for m in range(len(modes)):
            re = back[m * A : (m + 1) * A, :128]
            im = back[m * A : (m + 1) * A, 128:]
            real_rows.append(re * tw_r + im * tw_i)
            imag_rows.append(im * tw_r - re * tw_i)
        joined = jnp.concatenate(
            [jnp.concatenate(real_rows, axis=1), jnp.concatenate(imag_rows, axis=1)], axis=0
        )
        return left_dot(left_i, joined)

    def send_gradient(b, h, m, peer):
        rows = pl.ds(h * Hk, Hk)
        go(
            grads.at[b, peer * ml + m, :, rows], rows_back.at[b, m, me_m, :, rows],
            5, gb_r.at[b, m], "mode", peer,
        )

    def line_up(b):
        @pl.loop(0, M)
        def _(p):
            owner, local = p // ml, lax.rem(p, ml)
            for ri in range(2):
                wanted[p, ri] = jnp.concatenate(
                    [t2[b, j, owner, ri, pl.ds(local, As, stride=ml), :] for j in range(Dt)], axis=0
                )

    def each(count, body):
        if M <= 8:
            for i in range(count):
                body(i)
        else:
            pl.loop(0, count)(body)

    def span(start, size):
        return pl.ds(start if isinstance(start, int) else pl.multiple_of(start, size), size)

    def kerr(b, h):
        field = kb[b * parts + h]
        tiles = Hk // 8
        depth = J * 8

        def block(ref, row, q):
            return [ref[span(row * 8, 8), (2 * q + ri) * 128 : (2 * q + ri + 1) * 128] for ri in range(2)]

        def put(ref, start, q, ri, value):
            ref[span(start, 16), (2 * q + ri) * 128 : (2 * q + ri + 1) * 128] = value

        def multiply_pairs(q):
            here = pl.ds(q * 8, 8)
            for j in range(0, J, 2):
                made = []
                for s in range(2):
                    first, second = pairs[0, j + s], pairs[1, j + s]
                    ar, ai = field[first, 0, here], field[first, 1, here]
                    br, bi = field[second, 0, here], field[second, 1, here]
                    made.append((ar * br - ai * bi, ar * bi + ai * br))
                for ri in range(2):
                    high, low = halves(jnp.concatenate([value[ri] for value in made], axis=0))
                    for part, value in enumerate((high, low, high)):
                        put(pair_cols, part * depth + j * 8, q, ri, value)

        def couple(q):
            cols = pl.ds(q * 256, 256)
            coup[:, cols] = mm(w1[...], pair_cols[:, cols])

        def compare(q):
            rows, here = pl.ds(h * Hk + q * 8, 8), pl.ds(q * 8, 8)

            def body(pp):
                pushed = []
                for s in range(2):
                    p = pp * 2 + s
                    kr = ki = jnp.zeros((8, 128), f32)
                    for n in range(M):
                        cr, ci = block(coup, p * M + n, q)
                        ur, ui = field[n, 0, here], field[n, 1, here]
                        kr = kr + (cr * ur + ci * ui)
                        ki = ki + (ci * ur - cr * ui)
                    cr = 2.0 * (field[p, 0, here] - kerr_scale * ki - wanted[p, 0, rows])
                    ci = 2.0 * (field[p, 1, here] + kerr_scale * kr - wanted[p, 1, rows])
                    cots[p, 0, rows] = cr
                    cots[p, 1, rows] = ci
                    pushed.append((kerr_scale * ci, -kerr_scale * cr))
                    push[p, 0, rows] = pushed[s][0]
                    push[p, 1, rows] = pushed[s][1]
                for ri in range(2):
                    high, low = halves(jnp.concatenate([value[ri] for value in pushed], axis=0))
                    for part, value in enumerate((high, low, high)):
                        put(push_cols, part * (M * 8) + pp * 16, q, ri, value)

            each(M // 2, body)

        def turn_back(q):
            cols = pl.ds(q * 256, 256)
            turn[:, cols] = mm(w2[...], push_cols[:, cols])

        def through_conjugate(q):
            rows = pl.ds(h * Hk + q * 8, 8)

            def body(n):
                gr, gi = cots[n, 0, rows], cots[n, 1, rows]
                for p in range(M):
                    cr, ci = block(coup, p * M + n, q)
                    er, ei = push[p, 0, rows], push[p, 1, rows]
                    gr = gr + (er * cr + ei * ci)
                    gi = gi + (er * ci - ei * cr)
                direct[n, 0, rows] = gr
                direct[n, 1, rows] = gi

            each(M, body)

        def through_pairs(q):
            here = pl.ds(q * 8, 8)

            def body(jj):
                moved = [[], []]
                for s in range(2):
                    j = jj * 2 + s
                    gr = gi = jnp.zeros((8, 128), f32)
                    for n in range(M):
                        tr, ti = block(turn, n * J + j, q)
                        ur, ui = field[n, 0, here], field[n, 1, here]
                        gr = gr + (tr * ur - ti * ui)
                        gi = gi + (tr * ui + ti * ur)
                    for side in range(2):
                        other = pairs[1 - side, j]
                        vr, vi = field[other, 0, here], field[other, 1, here]
                        moved[side].append((vr * gr + vi * gi, vr * gi - vi * gr))
                for side in range(2):
                    for ri in range(2):
                        high, low = halves(jnp.concatenate([value[ri] for value in moved[side]], axis=0))
                        put(move_cols, side * depth + jj * 16, q, ri, high)
                        put(move_cols, (2 + side) * depth + jj * 16, q, ri, low)

            each(J // 2, body)

        def gather(q):
            rows = pl.ds(h * Hk + q * 8, 8)
            back = mm(spread[...], move_cols[:, q * 256 : q * 256 + 256])
            for n in range(M):
                for ri in range(2):
                    grads[b, n, ri, rows] = (
                        direct[n, ri, rows] + back[n * 8 : n * 8 + 8, ri * 128 : ri * 128 + 128]
                    )

        for q in range(tiles):
            multiply_pairs(q)
        for q in range(tiles):
            couple(q)
        for q in range(tiles):
            compare(q)
            turn_back(q)
        for q in range(tiles):
            through_conjugate(q)
            through_pairs(q)
            gather(q)

    for b in range(Bl):
        arrived(rows_in.at[b], in_r.at[b])
        stacked = jnp.concatenate(
            [
                jnp.concatenate(
                    [rows_in[b, j, ri, pl.ds(m, Al, stride=ml), :] for ri in range(2) for j in range(Dt)], axis=0
                )
                for m in range(ml)
            ],
            axis=1,
        )
        result = disperse(stacked, 1.0, range(ml))
        for i in range(Dm):
            for m in range(ml):
                for ri in range(2):
                    for j in range(Dt):
                        row = ri * A + j * Al + i * As
                        h, at = j * As // Hk, j * As % Hk
                        send_z[i, b, h, m, ri, at : at + As, :] = result[row : row + As, m * 128 : (m + 1) * 128]
        for h in range(parts):
            for peer in mode_peers[::-1]:
                go(
                    send_z.at[peer, b, h], kb[b * parts + h].at[pl.ds(me_m * ml, ml)],
                    4, kb_r.at[b, h], "mode", peer,
                )
            own(send_z.at[me_m, b, h], kb[b * parts + h].at[pl.ds(me_m * ml, ml)], kb_r.at[b, h])
        if b == 0:
            target_second_leg(0)

    arrived(mg, mg_r)
    make_weights(sizes, pairs, mg, w1, w2, spread)
    for b in range(1, Bl):
        target_second_leg(b)

    for b in range(Bl):
        arrived(t2.at[b], t2_r.at[b])
        line_up(b)
        for h in range(parts):
            arrived(kb[b * parts + h], kb_r.at[b, h])
            kerr(b, h)
            if b + 1 < Bl:
                for m in range(ml):
                    for peer in mode_peers:
                        send_gradient(b, h, m, peer)
        if b + 1 == Bl:
            for peer in mode_peers:
                for m in range(ml):
                    for h in range(parts):
                        send_gradient(b, h, m, peer)
        for m in range(ml):
            own(grads.at[b, me_m * ml + m], rows_back.at[b, m, me_m], gb_r.at[b, m])

    for b in range(Bl):
        for m in range(ml):
            arrived(rows_back.at[b, m], gb_r.at[b, m])
            stacked = jnp.concatenate(
                [
                    rows_back[b, m, i, ri, j * As : (j + 1) * As, :]
                    for ri in range(2)
                    for j in range(Dt)
                    for i in range(Dm)
                ],
                axis=0,
            )
            result = disperse(stacked, -1.0, [m])
            for j in range(Dt):
                for ri in range(2):
                    row = ri * A + j * Al
                    send_out[j, b, m, ri] = result[row : row + Al, :]
            for peer in tm_peers:
                go(
                    send_out.at[peer, b, m], out.at[:, me_t * Bl + b, m],
                    6, out_r, "tm", peer,
                )
            own(send_out.at[me_t, b, m], out.at[:, me_t * Bl + b, m], out_r)
    arrived(out, out_r)
    others_t, others_m = pl.ds(0, Dt - 1), pl.ds(0, Dm - 1)
    for leg, whole in enumerate(
        (
            rows_in.at[:, others_t],
            mg.at[others_m],
            t1.at[:, others_m],
            t2.at[:, others_t],
            send_z.at[others_m],
            rows_back.at[:, :, others_m],
            send_out.at[others_t],
        )
    ):
        arrived(whole, sent.at[leg])


def finish(gathered, out, sem):
    _, B, ml, _, _ = gathered.shape
    for b in range(B):
        for m in range(ml):
            pltpu.make_async_copy(gathered.at[:, b, m], out.at[:, b, :, m], sem).start()
    pltpu.make_async_copy(gathered, gathered, sem).wait()


def on_device(Dm, Dt, input_field, target_field, margin, pair_index, mode_beta, segment_kind):
    _, B, ml, Tl = input_field.shape
    M, J = margin.shape[1], margin.shape[2]
    total = Tl * Dt
    A = total // 128
    Al = Tl // 128
    Bl = B // Dt
    As = Al // Dm
    Ak = As * Dt
    parts = 2 if Ak % 16 == 0 else 1
    Hk = Ak // parts
    def by_rows(values):
        return values.reshape(2, B, ml, Al, 128).transpose(0, 1, 3, 2, 4).reshape(2, B, Al * ml, 128)

    x = by_rows(input_field)
    target = by_rows(target_field).reshape(2, Dt, Bl, Al * ml, 128)
    if (As * ml) % 8:
        target = target.reshape(2, Dt, Bl, Dm, As * ml, 128).transpose(3, 0, 1, 2, 4, 5)
    tables = make_tables(A, total)
    sizes = (Dt, Dm, B, Bl, ml, M, A, Al, As, Ak, J, total)
    vm = lambda *shape: pltpu.VMEM(shape, f32)
    vb = lambda *shape: pltpu.VMEM(shape, bf16)
    dma = lambda *shape: pltpu.SemaphoreType.DMA(shape)
    anyspace = pl.BlockSpec(memory_space=pl.ANY)
    gathered = pl.pallas_call(
        functools.partial(kernel, sizes),
        out_shape=pltpu.VMEM((2, B, ml, Al, 128), f32),
        in_specs=[anyspace] * 11,
        out_specs=anyspace,
        scratch_shapes=[
            vm(*x.shape),
            vm(*target.shape),
            pltpu.SMEM(segment_kind.shape, jnp.int32),
            pltpu.SMEM(pair_index.shape[::-1], jnp.int32),
            vm(ml, M, J),
        ]
        + [pltpu.VMEM(t.shape, bf16) for t in tables[:4]]
        + [
            vm(2, A, 128),
            pltpu.SMEM((3, ml, mode_beta.shape[0]), f32),
            vm(2, ml * A, 128),
            vm(Bl, Dt, 2, Al * ml, 128),
            vm(Dm, Bl, parts, ml, 2, Hk, 128),
            [vm(M, 2, Hk, 128) for _ in range(Bl * parts)],
            vm(Bl, Dm, 2, Dt, As * ml, 128),
            vm(Bl, Dt, Dm, 2, As * ml, 128),
            vm(Dm, ml, M, J),
            vb(M * M * 8, 3 * J * 8),
            vb(M * J * 8, 3 * M * 8),
            vb(M * 8, 4 * J * 8),
            vb(3 * J * 8, Hk * 32),
            vm(M * M * 8, Hk * 32),
            vm(M, 2, Ak, 128),
            vm(M, 2, Ak, 128),
            vm(M, 2, Ak, 128),
            vb(3 * M * 8, Hk * 32),
            vm(M * J * 8, Hk * 32),
            vm(M, 2, Ak, 128),
            vb(4 * J * 8, Hk * 32),
            vm(Bl, M, 2, Ak, 128),
            vm(Bl, ml, Dm, 2, Ak, 128),
            vm(Dt, Bl, ml, 2, Al, 128),
            dma(5),
            dma(6),
            dma(7),
            dma(Bl),
            dma(),
            dma(Bl),
            dma(Bl),
            dma(Bl, parts),
            dma(Bl, ml),
            dma(),
        ],
        compiler_params=pltpu.CompilerParams(collective_id=0, has_side_effects=True, vmem_limit_bytes=62 * 1024 * 1024),
    )(segment_kind, pair_index.T, x, target, margin, mode_beta.transpose(2, 1, 0), *[jnp.asarray(t) for t in tables])
    out = pl.pallas_call(
        finish,
        out_shape=jax.ShapeDtypeStruct((2, B, Al, ml, 128), f32),
        in_specs=[anyspace],
        out_specs=anyspace,
        scratch_shapes=[dma()],
    )(pltpu.with_memory_space_constraint(gathered, pltpu.VMEM))
    return out.transpose(0, 1, 3, 2, 4).reshape(2, B, ml, Tl)


def solution(mesh):
    return jax.shard_map(
        functools.partial(on_device, mesh.shape["mode"], mesh.shape["tm"]),
        mesh=mesh,
        in_specs=(
            P(None, "dp", "mode", "tm"),
            P(None, "dp", "mode", "tm"),
            P("mode", None, None),
            P(),
            P(None, "mode", None),
            P(),
        ),
        out_specs=P(None, "dp", "mode", "tm"),
        check_vma=False,
    )
```

```python
import functools
import math

import jax
import jax.numpy as jnp
import numpy as np
from jax import lax
from jax.experimental import pallas as pl
from jax.experimental.pallas import tpu as pltpu
from jax.sharding import PartitionSpec as P

kerr_scale = 0.1
MESH = pl.DeviceIdType.MESH
f32 = jnp.float32
bf16 = jnp.bfloat16


def split_table(table):
    high = table.astype(np.float32).astype(bf16)
    low = (table - high.astype(np.float64)).astype(np.float32).astype(bf16)
    return np.stack([np.asarray(high), np.asarray(low)])


def real_form(size):
    turns = np.outer(np.arange(size), np.arange(size)) % size
    angle = turns * (2.0 * math.pi / size)
    cosine, sine = np.cos(angle), np.sin(angle)
    return np.block([[cosine, sine], [-sine, cosine]])


def make_tables(outer, total):
    left, right = real_form(outer), real_form(128)
    turns = np.outer(np.arange(outer), np.arange(128)) % total
    angle = turns * (2.0 * math.pi / total)
    twist = np.stack([np.cos(angle), -np.sin(angle)]).astype(np.float32)
    return (
        split_table(left),
        split_table(left.T / total),
        split_table(right.T),
        split_table(right),
        twist,
    )


def halves(value):
    high = value.astype(bf16)
    return high, (value - high.astype(f32)).astype(bf16)


def mm(a, b):
    return jnp.dot(a, b, preferred_element_type=f32)


def left_dot(table, value):
    high, low = halves(value)
    width = value.shape[1]
    if width > 128:
        return mm(table[0], high) + (mm(table[0], low) + mm(table[1], high))
    both = mm(table[0], jnp.concatenate([high, low], axis=1))
    return both[:, :width] + (both[:, width:] + mm(table[1], high))


def right_dot(value, table):
    high, low = halves(value)
    rows = value.shape[0]
    both = mm(jnp.concatenate([high, low], axis=0), table[0])
    return both[:rows] + (both[rows:] + mm(high, table[1]))


def farthest_first(me, count):
    low, high = jnp.int32(0), jnp.int32(count - 1)
    peers = []
    for _ in range(count - 1):
        up = (high - me >= me - low).astype(jnp.int32)
        peers.append(up * high + (1 - up) * low)
        high, low = high - up, low + 1 - up
    return peers


def digits(shape, axis):
    return lax.broadcasted_iota(jnp.int32, shape, axis)


def one_hot(condition):
    return jnp.where(condition, 1.0, 0.0).astype(bf16)


def make_weights(sizes, pairs, mg, w1, w2, spread):
    Dt, Dm, B, Bl, ml, M, A, Al, As, Ak, J, total = sizes
    depth = J * 8
    group = max(1, 64 // M)
    step = group * M

    rows, cols = digits((step * 8, step), 0), digits((step * 8, step), 1)
    taller = one_hot(rows // 8 == cols)
    rows, cols = digits((2 * J, 3 * depth), 0), digits((2 * J, 3 * depth), 1)
    wider = one_hot((rows == cols % depth // 8 + jnp.where(cols < 2 * depth, 0, J)))
    kept = digits((step * 8, 3 * depth), 0) % 8 == digits((step * 8, 3 * depth), 1) % 8

    def block(p):
        return mg[p // ml, p % ml]

    columns = []
    for g in range(M // group):
        values = jnp.concatenate([block(g * group + i) for i in range(group)], axis=0)
        high, low = halves(values)
        both = jnp.concatenate([high.astype(f32), low.astype(f32)], axis=1).astype(bf16)
        tall = mm(taller, both).astype(bf16)
        wide = mm(tall, wider)
        w1[g * step * 8 : (g + 1) * step * 8, :] = jnp.where(kept, wide, 0.0).astype(bf16)
        columns.append((high, low))

    rows, cols = digits((depth, J), 0), digits((depth, J), 1)
    lifter = one_hot(rows // 8 == cols)

    def turned(values):
        return lax.dot_general(lifter, values, (((1,), (1,)), ((), ())), preferred_element_type=f32).astype(bf16)

    lifted = [[turned(part) for part in pair] for pair in columns]
    width = M * 8
    kept = digits((depth, 3 * width), 0) % 8 == digits((depth, 3 * width), 1) % 8
    rows, cols = digits((step, 3 * width), 0), digits((step, 3 * width), 1)

    def fill(n):
        total = jnp.zeros((depth, 3 * width), f32)
        for g, parts in enumerate(lifted):
            for which, part in enumerate(parts):
                inside = (cols >= 2 * width) if which else (cols < 2 * width)
                match = (rows // M + g * group == cols % width // 8) & (rows % M == n) & inside
                total = total + mm(part, one_hot(match))
        w2[pl.ds(pl.multiple_of(n * depth, depth), depth), :] = jnp.where(kept, total, 0.0).astype(bf16)

    if M <= 8:
        for n in range(M):
            fill(n)
    else:
        pl.loop(0, M)(fill)

    which = digits((8, 2 * depth), 1) // 8
    chosen = jnp.zeros((8, 2 * depth), jnp.int32)
    for side in range(2):
        for j in range(J):
            chosen = jnp.where(which == side * J + j, pairs[side, j], chosen)
    shape = (width, 2 * depth)
    match = (digits(shape, 0) // 8 == jnp.concatenate([chosen] * M, axis=0)) & (
        digits(shape, 0) % 8 == digits(shape, 1) % 8
    )
    spread[:, : 2 * depth] = one_hot(match)
    spread[:, 2 * depth :] = one_hot(match)


def kernel(
    sizes, kind_hbm, pairs_hbm, x, target, margin_hbm, beta_hbm,
    left_f_hbm, left_i_hbm, right_f_hbm, right_i_hbm, twist_hbm, out,
    x_near, target_near, kind, pairs, margin, left_f, left_i, right_f, right_i, twist, beta, phase_tab,
    rows_in, send_z, kb, t1, t2, mg, w1, w2, spread, pair_cols, coup, wanted, cots, push, push_cols, turn, direct, move_cols,
    grads, rows_back, send_out,
    near_sem, table_sem, sent, in_r, mg_r, t1_r, t2_r, kb_r, gb_r, out_r,
):
    Dt, Dm, B, Bl, ml, M, A, Al, As, Ak, J, total = sizes
    parts = 2 if Ak % 16 == 0 else 1
    Hk = Ak // parts
    me_t = lax.axis_index("tm")
    me_m = lax.axis_index("mode")
    tm_peers = farthest_first(me_t, Dt)
    mode_peers = farthest_first(me_m, Dm)

    def remote(src, dst, send, recv, axis, peer):
        return pltpu.make_async_remote_copy(
            src_ref=src, dst_ref=dst, send_sem=send, recv_sem=recv, device_id={axis: peer}, device_id_type=MESH
        )

    barrier = pltpu.get_barrier_semaphore()
    for peer in mode_peers:
        pl.semaphore_signal(barrier, inc=1, device_id={"mode": peer}, device_id_type=MESH)
    for peer in tm_peers:
        pl.semaphore_signal(barrier, inc=1, device_id={"tm": peer}, device_id_type=MESH)
    staged = []
    for spot, (src, dst) in enumerate(
        ((margin_hbm, margin), (target, target_near), (x, x_near), (kind_hbm, kind), (pairs_hbm, pairs))
    ):
        staged.append(pltpu.make_async_copy(src, dst, near_sem.at[spot]))
        staged[-1].start()
    pl.semaphore_wait(barrier, Dt + Dm - 2)

    def go(src, dst, leg, recv, axis, peer):
        remote(src, dst, sent.at[leg], recv, axis, peer).start()

    def own(src, dst, recv):
        pltpu.make_async_copy(src, dst, recv).start()

    def arrived(whole, recv):
        pltpu.make_async_copy(whole, whole, recv).wait()

    def target_part(i, b):
        if (As * ml) % 8 == 0:
            return target_near.at[:, :, b, pl.ds(pl.multiple_of(i * (As * ml), 8), As * ml), :]
        return target_near.at[i, :, :, b]

    def target_first_leg(b):
        for peer in mode_peers:
            go(target_part(peer, b), t1.at[b, me_m], 2, t1_r.at[b], "mode", peer)
        own(target_part(me_m, b), t1.at[b, me_m], t1_r.at[b])

    def target_second_leg(b):
        arrived(t1.at[b], t1_r.at[b])
        for peer in tm_peers:
            go(t1.at[b, :, :, peer], t2.at[b, me_t], 3, t2_r.at[b], "tm", peer)
        own(t1.at[b, :, :, me_t], t2.at[b, me_t], t2_r.at[b])

    staged[0].wait()
    for peer in mode_peers:
        go(margin, mg.at[me_m], 1, mg_r, "mode", peer)
    own(margin, mg.at[me_m], mg_r)
    staged[1].wait()
    target_first_leg(0)
    staged[2].wait()
    for b in range(Bl):
        for peer in tm_peers:
            go(x_near.at[:, peer * Bl + b], rows_in.at[b, me_t], 0, in_r.at[b], "tm", peer)
        own(x_near.at[:, me_t * Bl + b], rows_in.at[b, me_t], in_r.at[b])
    for b in range(1, Bl):
        target_first_leg(b)
    for copy in staged[3:]:
        copy.wait()
    table_copies = []
    for spot, (src, dst) in enumerate(
        ((left_f_hbm, left_f), (left_i_hbm, left_i), (right_f_hbm, right_f), (right_i_hbm, right_i), (twist_hbm, twist), (beta_hbm, beta))
    ):
        copy = pltpu.make_async_copy(src, dst, table_sem.at[spot])
        copy.start()
        table_copies.append(copy)

    for copy in table_copies:
        copy.wait()
    low_digit = lax.broadcasted_iota(jnp.int32, (A, 128), 0)
    high_digit = lax.broadcasted_iota(jnp.int32, (A, 128), 1)
    frequency = low_digit + A * high_digit
    signed = jnp.where(frequency < total // 2, frequency, frequency - total).astype(f32)
    omega = signed * (8.0 / total)
    for m in range(ml):
        phase = (
            beta[0, m, kind[0]] * omega
            + beta[1, m, kind[0]] * (omega * omega) / 2.0
            + beta[2, m, kind[0]] * (omega * omega * omega) / 6.0
        )
        phase_tab[0, m * A : (m + 1) * A, :] = jnp.cos(phase)
        phase_tab[1, m * A : (m + 1) * A, :] = jnp.sin(phase)
    def disperse(stacked, direction, modes):
        spun = left_dot(left_f, stacked)
        tw_r, tw_i = twist[0], twist[1]
        blocks = []
        for m in range(len(modes)):
            re = spun[:A, m * 128 : (m + 1) * 128]
            im = spun[A:, m * 128 : (m + 1) * 128]
            blocks.append(jnp.concatenate([re * tw_r - im * tw_i, re * tw_i + im * tw_r], axis=1))
        spectrum = right_dot(jnp.concatenate(blocks, axis=0), right_f)
        re, im = spectrum[:, :128], spectrum[:, 128:]
        cosine, sine = (
            jnp.concatenate([phase_tab[part, m * A : (m + 1) * A, :] for m in modes], axis=0) for part in range(2)
        )
        sine = sine * direction
        turned = jnp.concatenate([re * cosine - im * sine, re * sine + im * cosine], axis=1)
        back = right_dot(turned, right_i)
        real_rows, imag_rows = [], []
        for m in range(len(modes)):
            re = back[m * A : (m + 1) * A, :128]
            im = back[m * A : (m + 1) * A, 128:]
            real_rows.append(re * tw_r + im * tw_i)
            imag_rows.append(im * tw_r - re * tw_i)
        joined = jnp.concatenate(
            [jnp.concatenate(real_rows, axis=1), jnp.concatenate(imag_rows, axis=1)], axis=0
        )
        return left_dot(left_i, joined)

    def send_gradient(b, h, m, peer):
        rows = pl.ds(h * Hk, Hk)
        go(
            grads.at[b, peer * ml + m, :, rows], rows_back.at[b, m, me_m, :, rows],
            5, gb_r.at[b, m], "mode", peer,
        )

    def line_up(b):
        @pl.loop(0, M)
        def _(p):
            owner, local = p // ml, lax.rem(p, ml)
            for ri in range(2):
                wanted[p, ri] = jnp.concatenate(
                    [t2[b, j, owner, ri, pl.ds(local, As, stride=ml), :] for j in range(Dt)], axis=0
                )

    def each(count, body):
        if M <= 8:
            for i in range(count):
                body(i)
        else:
            pl.loop(0, count)(body)

    def span(start, size):
        return pl.ds(start if isinstance(start, int) else pl.multiple_of(start, size), size)

    def kerr(b, h):
        field = kb[b * parts + h]
        tiles = Hk // 8
        depth = J * 8

        def block(ref, row, q):
            return [ref[span(row * 8, 8), (2 * q + ri) * 128 : (2 * q + ri + 1) * 128] for ri in range(2)]

        def put(ref, start, q, ri, value):
            ref[span(start, 16), (2 * q + ri) * 128 : (2 * q + ri + 1) * 128] = value

        def multiply_pairs(q):
            here = pl.ds(q * 8, 8)
            for j in range(0, J, 2):
                made = []
                for s in range(2):
                    first, second = pairs[0, j + s], pairs[1, j + s]
                    ar, ai = field[first, 0, here], field[first, 1, here]
                    br, bi = field[second, 0, here], field[second, 1, here]
                    made.append((ar * br - ai * bi, ar * bi + ai * br))
                for ri in range(2):
                    high, low = halves(jnp.concatenate([value[ri] for value in made], axis=0))
                    for part, value in enumerate((high, low, high)):
                        put(pair_cols, part * depth + j * 8, q, ri, value)

        def couple(q):
            cols = pl.ds(q * 256, 256)
            coup[:, cols] = mm(w1[...], pair_cols[:, cols])

        def compare(q):
            rows, here = pl.ds(h * Hk + q * 8, 8), pl.ds(q * 8, 8)

            def body(pp):
                pushed = []
                for s in range(2):
                    p = pp * 2 + s
                    kr = ki = jnp.zeros((8, 128), f32)
                    for n in range(M):
                        cr, ci = block(coup, p * M + n, q)
                        ur, ui = field[n, 0, here], field[n, 1, here]
                        kr = kr + (cr * ur + ci * ui)
                        ki = ki + (ci * ur - cr * ui)
                    cr = 2.0 * (field[p, 0, here] - kerr_scale * ki - wanted[p, 0, rows])
                    ci = 2.0 * (field[p, 1, here] + kerr_scale * kr - wanted[p, 1, rows])
                    cots[p, 0, rows] = cr
                    cots[p, 1, rows] = ci
                    pushed.append((kerr_scale * ci, -kerr_scale * cr))
                    push[p, 0, rows] = pushed[s][0]
                    push[p, 1, rows] = pushed[s][1]
                for ri in range(2):
                    high, low = halves(jnp.concatenate([value[ri] for value in pushed], axis=0))
                    for part, value in enumerate((high, low, high)):
                        put(push_cols, part * (M * 8) + pp * 16, q, ri, value)

            each(M // 2, body)

        def turn_back(q):
            cols = pl.ds(q * 256, 256)
            turn[:, cols] = mm(w2[...], push_cols[:, cols])

        def through_conjugate(q):
            rows = pl.ds(h * Hk + q * 8, 8)

            def body(n):
                gr, gi = cots[n, 0, rows], cots[n, 1, rows]
                for p in range(M):
                    cr, ci = block(coup, p * M + n, q)
                    er, ei = push[p, 0, rows], push[p, 1, rows]
                    gr = gr + (er * cr + ei * ci)
                    gi = gi + (er * ci - ei * cr)
                direct[n, 0, rows] = gr
                direct[n, 1, rows] = gi

            each(M, body)

        def through_pairs(q):
            here = pl.ds(q * 8, 8)

            def body(jj):
                moved = [[], []]
                for s in range(2):
                    j = jj * 2 + s
                    gr = gi = jnp.zeros((8, 128), f32)
                    for n in range(M):
                        tr, ti = block(turn, n * J + j, q)
                        ur, ui = field[n, 0, here], field[n, 1, here]
                        gr = gr + (tr * ur - ti * ui)
                        gi = gi + (tr * ui + ti * ur)
                    for side in range(2):
                        other = pairs[1 - side, j]
                        vr, vi = field[other, 0, here], field[other, 1, here]
                        moved[side].append((vr * gr + vi * gi, vr * gi - vi * gr))
                for side in range(2):
                    for ri in range(2):
                        high, low = halves(jnp.concatenate([value[ri] for value in moved[side]], axis=0))
                        put(move_cols, side * depth + jj * 16, q, ri, high)
                        put(move_cols, (2 + side) * depth + jj * 16, q, ri, low)

            each(J // 2, body)

        def gather(q):
            rows = pl.ds(h * Hk + q * 8, 8)
            back = mm(spread[...], move_cols[:, q * 256 : q * 256 + 256])
            for n in range(M):
                for ri in range(2):
                    grads[b, n, ri, rows] = (
                        direct[n, ri, rows] + back[n * 8 : n * 8 + 8, ri * 128 : ri * 128 + 128]
                    )

        for q in range(tiles):
            multiply_pairs(q)
        for q in range(tiles):
            couple(q)
        for q in range(tiles):
            compare(q)
            turn_back(q)
        for q in range(tiles):
            through_conjugate(q)
            through_pairs(q)
            gather(q)

    for b in range(Bl):
        arrived(rows_in.at[b], in_r.at[b])
        stacked = jnp.concatenate(
            [
                jnp.concatenate(
                    [rows_in[b, j, ri, pl.ds(m, Al, stride=ml), :] for ri in range(2) for j in range(Dt)], axis=0
                )
                for m in range(ml)
            ],
            axis=1,
        )
        result = disperse(stacked, 1.0, range(ml))
        for i in range(Dm):
            for m in range(ml):
                for ri in range(2):
                    for j in range(Dt):
                        row = ri * A + j * Al + i * As
                        h, at = j * As // Hk, j * As % Hk
                        send_z[i, b, h, m, ri, at : at + As, :] = result[row : row + As, m * 128 : (m + 1) * 128]
        for h in range(parts):
            for peer in mode_peers[::-1]:
                go(
                    send_z.at[peer, b, h], kb[b * parts + h].at[pl.ds(me_m * ml, ml)],
                    4, kb_r.at[b, h], "mode", peer,
                )
            own(send_z.at[me_m, b, h], kb[b * parts + h].at[pl.ds(me_m * ml, ml)], kb_r.at[b, h])

    arrived(mg, mg_r)
    make_weights(sizes, pairs, mg, w1, w2, spread)
    for b in range(Bl):
        target_second_leg(b)

    for b in range(Bl):
        arrived(t2.at[b], t2_r.at[b])
        line_up(b)
        for h in range(parts):
            arrived(kb[b * parts + h], kb_r.at[b, h])
            kerr(b, h)
            if b + 1 < Bl:
                for m in range(ml):
                    for peer in mode_peers:
                        send_gradient(b, h, m, peer)
        if b + 1 == Bl:
            for peer in mode_peers:
                for m in range(ml):
                    for h in range(parts):
                        send_gradient(b, h, m, peer)
        for m in range(ml):
            own(grads.at[b, me_m * ml + m], rows_back.at[b, m, me_m], gb_r.at[b, m])

    for b in range(Bl):
        for m in range(ml):
            arrived(rows_back.at[b, m], gb_r.at[b, m])
            stacked = jnp.concatenate(
                [
                    rows_back[b, m, i, ri, j * As : (j + 1) * As, :]
                    for ri in range(2)
                    for j in range(Dt)
                    for i in range(Dm)
                ],
                axis=0,
            )
            result = disperse(stacked, -1.0, [m])
            for j in range(Dt):
                for ri in range(2):
                    row = ri * A + j * Al
                    send_out[j, b, m, ri] = result[row : row + Al, :]
            for peer in tm_peers:
                go(
                    send_out.at[peer, b, m], out.at[:, me_t * Bl + b, m],
                    6, out_r, "tm", peer,
                )
            own(send_out.at[me_t, b, m], out.at[:, me_t * Bl + b, m], out_r)
    arrived(out, out_r)
    others_t, others_m = pl.ds(0, Dt - 1), pl.ds(0, Dm - 1)
    for leg, whole in enumerate(
        (
            rows_in.at[:, others_t],
            mg.at[others_m],
            t1.at[:, others_m],
            t2.at[:, others_t],
            send_z.at[others_m],
            rows_back.at[:, :, others_m],
            send_out.at[others_t],
        )
    ):
        arrived(whole, sent.at[leg])


def finish(gathered, out, sem):
    _, B, ml, _, _ = gathered.shape
    for b in range(B):
        for m in range(ml):
            pltpu.make_async_copy(gathered.at[:, b, m], out.at[:, b, :, m], sem).start()
    pltpu.make_async_copy(gathered, gathered, sem).wait()


def on_device(Dm, Dt, input_field, target_field, margin, pair_index, mode_beta, segment_kind):
    _, B, ml, Tl = input_field.shape
    M, J = margin.shape[1], margin.shape[2]
    total = Tl * Dt
    A = total // 128
    Al = Tl // 128
    Bl = B // Dt
    As = Al // Dm
    Ak = As * Dt
    parts = 2 if Ak % 16 == 0 else 1
    Hk = Ak // parts
    def by_rows(values):
        return values.reshape(2, B, ml, Al, 128).transpose(0, 1, 3, 2, 4).reshape(2, B, Al * ml, 128)

    x = by_rows(input_field)
    target = by_rows(target_field).reshape(2, Dt, Bl, Al * ml, 128)
    if (As * ml) % 8:
        target = target.reshape(2, Dt, Bl, Dm, As * ml, 128).transpose(3, 0, 1, 2, 4, 5)
    tables = make_tables(A, total)
    sizes = (Dt, Dm, B, Bl, ml, M, A, Al, As, Ak, J, total)
    vm = lambda *shape: pltpu.VMEM(shape, f32)
    vb = lambda *shape: pltpu.VMEM(shape, bf16)
    dma = lambda *shape: pltpu.SemaphoreType.DMA(shape)
    anyspace = pl.BlockSpec(memory_space=pl.ANY)
    gathered = pl.pallas_call(
        functools.partial(kernel, sizes),
        out_shape=pltpu.VMEM((2, B, ml, Al, 128), f32),
        in_specs=[anyspace] * 11,
        out_specs=anyspace,
        scratch_shapes=[
            vm(*x.shape),
            vm(*target.shape),
            pltpu.SMEM(segment_kind.shape, jnp.int32),
            pltpu.SMEM(pair_index.shape[::-1], jnp.int32),
            vm(ml, M, J),
        ]
        + [pltpu.VMEM(t.shape, bf16) for t in tables[:4]]
        + [
            vm(2, A, 128),
            pltpu.SMEM((3, ml, mode_beta.shape[0]), f32),
            vm(2, ml * A, 128),
            vm(Bl, Dt, 2, Al * ml, 128),
            vm(Dm, Bl, parts, ml, 2, Hk, 128),
            [vm(M, 2, Hk, 128) for _ in range(Bl * parts)],
            vm(Bl, Dm, 2, Dt, As * ml, 128),
            vm(Bl, Dt, Dm, 2, As * ml, 128),
            vm(Dm, ml, M, J),
            vb(M * M * 8, 3 * J * 8),
            vb(M * J * 8, 3 * M * 8),
            vb(M * 8, 4 * J * 8),
            vb(3 * J * 8, Hk * 32),
            vm(M * M * 8, Hk * 32),
            vm(M, 2, Ak, 128),
            vm(M, 2, Ak, 128),
            vm(M, 2, Ak, 128),
            vb(3 * M * 8, Hk * 32),
            vm(M * J * 8, Hk * 32),
            vm(M, 2, Ak, 128),
            vb(4 * J * 8, Hk * 32),
            vm(Bl, M, 2, Ak, 128),
            vm(Bl, ml, Dm, 2, Ak, 128),
            vm(Dt, Bl, ml, 2, Al, 128),
            dma(5),
            dma(6),
            dma(7),
            dma(Bl),
            dma(),
            dma(Bl),
            dma(Bl),
            dma(Bl, parts),
            dma(Bl, ml),
            dma(),
        ],
        compiler_params=pltpu.CompilerParams(collective_id=0, has_side_effects=True, vmem_limit_bytes=62 * 1024 * 1024),
    )(segment_kind, pair_index.T, x, target, margin, mode_beta.transpose(2, 1, 0), *[jnp.asarray(t) for t in tables])
    out = pl.pallas_call(
        finish,
        out_shape=jax.ShapeDtypeStruct((2, B, Al, ml, 128), f32),
        in_specs=[anyspace],
        out_specs=anyspace,
        scratch_shapes=[dma()],
    )(pltpu.with_memory_space_constraint(gathered, pltpu.VMEM))
    return out.transpose(0, 1, 3, 2, 4).reshape(2, B, ml, Tl)


def solution(mesh):
    return jax.shard_map(
        functools.partial(on_device, mesh.shape["mode"], mesh.shape["tm"]),
        mesh=mesh,
        in_specs=(
            P(None, "dp", "mode", "tm"),
            P(None, "dp", "mode", "tm"),
            P("mode", None, None),
            P(),
            P(None, "mode", None),
            P(),
        ),
        out_specs=P(None, "dp", "mode", "tm"),
        check_vma=False,
    )
```
